512 devices in a mesh: img: 16 (over z), sy: 8 (over x, core), sx: 4 (over y).
Axes of the slice: x: 4, y: 4, z: 16, core: 2. Of those that a mesh axis runs over, the one named last changes fastest.
Arguments:
- memory: bfloat16 [32, 81920, 256], P('img', ('sy', 'sx')), may hold values from -6 to 6
- enc_weight: bfloat16 [256, 256], replicated, may hold values from -0.375 to 0.375
- enc_bias: float32 [256], replicated, may hold values from -4 to 4
- norm_gain: float32 [256], replicated, may hold values from 0.25 to 1.75
- norm_bias: float32 [256], replicated, may hold values from -3 to 3
- class_weight: bfloat16 [256, 91], replicated, may hold values from -0.375 to 0.375
- class_bias: float32 [91], replicated, may hold values from -4 to 4
- box_w1: bfloat16 [256, 256], replicated, may hold values from -0.375 to 0.375
- box_b1: float32 [256], replicated, may hold values from -3 to 3
- box_w2: bfloat16 [256, 256], replicated, may hold values from -0.375 to 0.375
- box_b2: float32 [256], replicated, may hold values from -3 to 3
- box_w3: bfloat16 [256, 4], replicated, may hold values from -0.375 to 0.375
- box_b3: float32 [4], replicated, may hold values from -3 to 3
- picked: int32 [32, 1280], P('img', ('sy', 'sx')), may hold values from 0 to 2559, as said below
- counts: int32 [32, 32], P('img', ('sy', 'sx')), may hold values from 1 to 40, 320 in all within a row
Outputs:
- token_logits: bfloat16 [32, 91, 81920], P('img', None, ('sy', 'sx'))
- token_boxes: float32 [32, 4, 81920], P('img', None, ('sy', 'sx'))
- query_feat: bfloat16 [32, 320, 256], P(None, 'img')
- query_logits: bfloat16 [32, 320, 91], P(None, 'img')
- query_boxes: bfloat16 [32, 320, 4], P(None, 'img')
The draws below stay inside these ranges and needn't reach their ends.
Inputs may be any that keep to these rules, and one draw needn't show every extreme that they name: `picked`: each tile's 40 entries are distinct local token indices in rising order; only the first counts of them are selected. Each image's counts sum to 320.
All inputs are finite; a program needn't handle non-finite values. No bound on the sum of `counts` on one device may be relied on, other than what follows from the above.
Results may differ from the reference program's by a relative error of at most 0.0041.
Values may be sent and summed in bfloat16 or wider, within the bound.
No kernel may reach another device: no remote copies, remote signals or barrier semaphores. Data moves between devices by JAX's collectives and lax.ppermute only.
A program may use at most 64 MiB of HBM per device.

```python
import math
import jax
import jax.numpy as jnp
import numpy as np
from jax import lax

D = 256
CLS = 91
TILE_H = 40
TILE_W = 64
TOK_DEV = 2560
SHARDS = 32
B = 32
TOKENS = 81920
QUERIES = 320
MOST = 40
N_SY = 8
N_SX = 4


def draw_picked(key, part):
    keys = jax.random.split(jax.random.fold_in(key, 7), B * SHARDS)

    def subset(single):
        return jnp.sort(jax.random.permutation(single, TOK_DEV)[:MOST])
    chosen = jax.vmap(subset)(keys)
    return chosen.reshape(B, SHARDS * MOST).astype(jnp.int32)


def level_of(key, dims, cuts, least, high):
    def one(position, shards_of):
        steps = jax.random.uniform(jax.random.fold_in(jax.random.fold_in(key, 6), position), (shards_of,), jnp.float32, least / len(cuts), high / len(cuts))
        return jnp.repeat(jnp.exp(steps), dims[position] // shards_of).reshape((-1,) + (1,) * (len(dims) - position - 1))

    loudness = one(*cuts[0])
    for cut in cuts[1:]:
        loudness = loudness * one(*cut)
    return loudness


def length_profile(count, total, most, lean):
    portions = [(1 << 20) // math.isqrt(rank ** lean) + 1 for rank in range(2, count + 1)]
    rest, given = total - most - (count - 1), [1] * (count - 1)
    while rest > 0:
        movable = [i for i in range(count - 1) if given[i] < most]
        whole, left = sum([portions[i] for i in movable]), rest
        for i in movable:
            addition = min(most - given[i], max(1, left * portions[i] // whole), rest)
            given[i] = given[i] + addition
            rest = rest - addition
    return np.array([most] + given)


def uneven(own_key, number_of, total, reach, skew):
    if number_of == 2:
        one = jax.random.randint(own_key, (), max(1, total - reach), min(reach, total - 1) + 1)
        return jnp.stack([one, total - one])
    sizes = jnp.asarray(length_profile(number_of, total, reach, skew), jnp.int32)
    couples = (number_of - 1) // 2
    donor, taker = sizes[1:1 + 2 * couples:2], sizes[2:2 + 2 * couples:2]
    slack = jnp.minimum(donor - 1, reach - taker)
    moved = jax.random.randint(jax.random.fold_in(own_key, 1), (couples,), 0, 1 << 20) % (slack + 1)
    sizes = sizes.at[1:1 + 2 * couples:2].set(donor - moved).at[2:2 + 2 * couples:2].set(taker + moved)
    return sizes[jax.random.permutation(jax.random.fold_in(own_key, 2), number_of)]


def noise(key, extent, width, bound, cuts=(), kind=jnp.bfloat16):
    loudness = level_of(key, extent, cuts, -0.22, 0.18) if cuts else 1.0
    drawn = jax.random.normal(key, extent, jnp.float32) * width * loudness
    return jnp.minimum(jnp.maximum(drawn, -bound), bound).astype(kind)


def setup_inputs(seed: int = 0) -> dict:
    streams_of = jax.random.split(jax.random.key(seed), 16)
    return {
        "memory": noise(streams_of[0], (B, TOKENS, D), 1.0, 6.0, ((0, 16), (1, 32))),
        "enc_weight": noise(streams_of[1], (D, D), D ** -0.5, 0.375),
        "enc_bias": noise(streams_of[2], (D,), 1.0, 4.0, (), jnp.float32),
        "norm_gain": jnp.clip(1.0 + 0.15 * jax.random.normal(streams_of[3], (D,), jnp.float32), 0.25, 1.75),
        "norm_bias": noise(streams_of[4], (D,), 0.5, 3.0, (), jnp.float32),
        "class_weight": noise(streams_of[5], (D, CLS), D ** -0.5, 0.375),
        "class_bias": noise(streams_of[6], (CLS,), 1.0, 4.0, (), jnp.float32),
        "box_w1": noise(streams_of[7], (D, D), D ** -0.5, 0.375),
        "box_b1": noise(streams_of[8], (D,), 0.5, 3.0, (), jnp.float32),
        "box_w2": noise(streams_of[9], (D, D), D ** -0.5, 0.375),
        "box_b2": noise(streams_of[10], (D,), 0.5, 3.0, (), jnp.float32),
        "box_w3": noise(streams_of[11], (D, 4), D ** -0.5, 0.375),
        "box_b3": noise(streams_of[12], (4,), 0.5, 3.0, (), jnp.float32),
        "picked": draw_picked(jax.random.fold_in(streams_of[15], 71), 0),
        "counts": jax.vmap(lambda own: uneven(own, SHARDS, QUERIES, MOST, 2))(jax.random.split(streams_of[14], B)).reshape((B, SHARDS)).astype(jnp.int32),
    }


def reference(memory, enc_weight, enc_bias, norm_gain, norm_bias, class_weight, class_bias, box_w1, box_b1, box_w2, box_b2, box_w3, box_b3, picked, counts):
    index = jnp.arange(TOKENS).astype(jnp.int32)
    tile = index // TOK_DEV
    local = index % TOK_DEV
    row = tile // N_SX * TILE_H + local // TILE_W
    col = tile % N_SX * TILE_W + local % TILE_W
    center_x = (col.astype(jnp.float32) + 0.5) / (TILE_W * N_SX)
    center_y = (row.astype(jnp.float32) + 0.5) / (TILE_H * N_SY)
    sizes_wh = jnp.full((TOKENS,), 0.05, jnp.float32)
    prior = jnp.stack([center_x, center_y, sizes_wh, sizes_wh])
    prior_logit = jnp.log(prior / (1.0 - prior))

    def heads(mem):
        pre = jnp.dot(mem, enc_weight, preferred_element_type=jnp.float32) + enc_bias
        mean = lax.optimization_barrier(jnp.mean(pre, axis=-1, keepdims=True))
        centered = pre - mean
        var = lax.optimization_barrier(jnp.mean(centered * centered, axis=-1, keepdims=True))
        out_mem = (centered * lax.rsqrt(var + 1e-05) * norm_gain + norm_bias).astype(jnp.bfloat16)
        logits = (jnp.dot(out_mem, class_weight, preferred_element_type=jnp.float32) + class_bias).astype(jnp.bfloat16).T
        hidden = jax.nn.relu(jnp.dot(out_mem, box_w1, preferred_element_type=jnp.float32) + box_b1).astype(jnp.bfloat16)
        hidden = jax.nn.relu(jnp.dot(hidden, box_w2, preferred_element_type=jnp.float32) + box_b2).astype(jnp.bfloat16)
        delta = jnp.dot(hidden, box_w3, preferred_element_type=jnp.float32) + box_b3
        boxes = jax.nn.sigmoid(delta.T + prior_logit)
        return (out_mem, logits, boxes)
    out_mem, token_logits, token_boxes = lax.map(heads, memory)

    def choose(out_one, logit_one, box_one, pick_one, count_one):
        starts = jnp.cumsum(count_one) - count_one
        steps = jnp.arange(MOST).astype(jnp.int32)
        slot = starts[:, None] + steps[None, :]
        valid = steps[None, :] < count_one[:, None]
        slot = jnp.where(valid, slot, QUERIES).astype(jnp.int32)
        token = (jnp.arange(SHARDS).astype(jnp.int32) * TOK_DEV)[:, None] + pick_one.reshape(SHARDS, MOST)
        chosen = jnp.zeros((QUERIES,), jnp.int32).at[slot.reshape(-1)].set(token.reshape(-1).astype(jnp.int32), mode='drop')
        return (out_one[chosen], logit_one[:, chosen].T, box_one[:, chosen].T.astype(jnp.bfloat16))
    query_feat, query_logits, query_boxes = jax.vmap(choose)(out_mem, token_logits, token_boxes, picked, counts)
    return (token_logits, token_boxes, query_feat, query_logits, query_boxes)
```

```python
import jax
import jax.numpy as jnp
from jax import lax
from jax.experimental import pallas as pl
from jax.experimental.pallas import tpu as pltpu
from jax.sharding import Mesh
from jax.sharding import PartitionSpec as P

TILE_H = 40
TILE_W = 64
D = 256
CLS = 91
KEYS = 4
MOST = 40
TOK = 2560
Q_DEV = 20
LANES = 128
ROWS = 24
BLOCK = 512
PLANE = ("sy_0", "sy_1", "sx")
CHIPS = ("sy_0", "sx")
F32 = jnp.float32
BF16 = jnp.bfloat16
VMEM = pl.BlockSpec(memory_space=pltpu.VMEM)
SMEM = pl.BlockSpec(memory_space=pltpu.SMEM)
ANY = pl.BlockSpec(memory_space=pl.ANY)
NT = (((1,), (1,)), ((), ()))


def near(x):
    return pltpu.with_memory_space_constraint(x, pltpu.VMEM)


def dot(a, b):
    return jnp.dot(a, b, preferred_element_type=F32)


def dot_nt(a, b):
    return lax.dot_general(a, b, NT, preferred_element_type=F32)


def column(v):
    n = v.shape[1]
    if n < LANES:
        v = jnp.concatenate([v, jnp.zeros((1, LANES - n), F32)], axis=1)
    return jnp.broadcast_to(v, (LANES, LANES)).T


def heads(x, enc_w, enc_b, gain, bias, cls_t, cls_b, w1, b1, w2, b2, w3_t, b3, prior_logit):
    pre = dot(x, enc_w[...]) + enc_b[...]
    mean = jnp.mean(pre, axis=-1, keepdims=True)
    centered = pre - mean
    var = jnp.mean(centered * centered, axis=-1, keepdims=True)
    out = (centered * lax.rsqrt(var + 1e-05) * gain[...] + bias[...]).astype(BF16)
    n = x.shape[0]
    cls_col = column(cls_b[...])[:CLS]
    if n > LANES:
        cls_col = jnp.concatenate([cls_col] * (n // LANES), axis=1)
    logits = (dot_nt(cls_t[...], out) + cls_col).astype(BF16)
    hidden = jnp.maximum(dot(out, w1[...]) + b1[...], 0.0).astype(BF16)
    hidden = jnp.maximum(dot(hidden, w2[...]) + b2[...], 0.0).astype(BF16)
    which = lax.broadcasted_iota(jnp.int32, (KEYS, n), 0)
    b3_col = jnp.where(which == 0, b3[0], jnp.where(which == 1, b3[1], jnp.where(which == 2, b3[2], b3[3])))
    delta = dot_nt(w3_t[...], hidden) + b3_col
    boxes = jax.nn.sigmoid(delta + prior_logit)
    return out, logits, boxes


def prior_logits(token, shard, map_w, map_h, cols_axis):
    row = shard // cols_axis * TILE_H + (token >> 6)
    col = shard % cols_axis * TILE_W + (token & 63)
    center_x = (col.astype(F32) + 0.5) / map_w
    center_y = (row.astype(F32) + 0.5) / map_h
    n = token.shape[1]
    which = lax.broadcasted_iota(jnp.int32, (4, n), 0)
    prior = jnp.where(which == 0, center_x, jnp.where(which == 1, center_y, 0.05))
    return jnp.log(prior / (1.0 - prior))


def select_body(cols_axis, map_w, map_h, chips, cores, picked, counts, shard, pick_vec, memory, *refs):
    weights, (payload, tiles) = refs[:12], refs[12:]
    for i in range(2):
        for k in range(MOST):
            base = pl.multiple_of((picked[i, k] >> 4) << 4, 16)
            j = i * MOST + k
            tiles[16 * j : 16 * j + 16, :] = memory[i, pl.ds(base, 16), :]
    n = 2 * MOST * 16
    row = lax.broadcasted_iota(jnp.int32, (LANES, n), 0)
    col = lax.broadcasted_iota(jnp.int32, (LANES, n), 1)
    pick = pick_vec[...]
    pick = jnp.concatenate([pick[0:1], pick[1:2], jnp.zeros((1, LANES - 2 * MOST), jnp.int32)], axis=1)
    pick_col = column((pick & 15).astype(F32)).astype(jnp.int32)
    pick_col = jnp.concatenate([pick_col] * (n // LANES), axis=1)
    chosen = col == row * 16 + pick_col
    x = dot(jnp.where(chosen, 1.0, 0.0).astype(BF16), tiles[...]).astype(BF16)
    prior = prior_logits(pick, shard[0], map_w, map_h, cols_axis)
    out, logits, boxes = heads(x, *weights, prior)
    out_t = out.astype(F32).T
    c0 = counts[0, 0].astype(F32)
    c1 = counts[0, 1].astype(F32)

    def marked(v):
        lane = lax.broadcasted_iota(jnp.int32, v.shape, 1)
        return jnp.where(lane == 80, c0, jnp.where(lane == 81, c1, v)).astype(BF16)

    out_t = marked(out_t)
    rest = jnp.concatenate(
        [logits.astype(F32), boxes.astype(F32), jnp.zeros((LANES - CLS - 4, LANES), F32)], axis=0
    )
    rest = marked(rest)
    for hi in range(chips // cols_axis):
        for lo in range(cols_axis):
            c = hi * cols_axis + lo
            for core in range(cores):
                p = (hi * cores + core) * cols_axis + lo
                payload[p, 0:16, :] = out_t[16 * c : 16 * c + 16, :]
                payload[p, 16:24, :] = rest[8 * c : 8 * c + 8, :]


def place_body(owners, received, after, messages, placed):
    shards = received.shape[0]
    flat = received[...].reshape(shards * ROWS, LANES)
    r = lax.broadcasted_iota(jnp.int32, (2 * shards, shards * ROWS), 0)
    m = lax.broadcasted_iota(jnp.int32, (2 * shards, shards * ROWS), 1)
    tile = (m * 2731) >> 16
    wanted = ((r < shards) & (tile == r)) | (tile < r - shards)
    take = jnp.where(wanted & (m == tile * ROWS), 1.0, 0.0)
    res = dot(take.astype(BF16), flat)
    count, start = res[:shards], res[shards:]
    lane = lax.broadcasted_iota(jnp.int32, (shards, LANES), 1)
    image = jnp.where(lane < MOST, 0, 1)
    step = lane - image * MOST
    pick = lambda a: jnp.where(lane < MOST, a[:, 80:81], a[:, 81:82]).astype(jnp.int32)
    slot = pick(start) + step
    valid = (step < pick(count)) & (lane < 2 * MOST)
    owner = (slot * 3277) >> 16
    place = owner * (2 * Q_DEV) + image * Q_DEV + (slot - owner * Q_DEV)
    place = jnp.where(valid, place, -1)
    total = owners * 2 * Q_DEV
    target = lax.broadcasted_iota(jnp.int32, (total, LANES), 0)
    acc = jnp.zeros((ROWS, total), F32)
    for t in range(0, shards, 2):
        hot = [jnp.where(target == place[u : u + 1], 1.0, 0.0).astype(BF16) for u in (t, t + 1)]
        lhs = jnp.concatenate([received[t], received[t + 1]], axis=1)
        acc = acc + dot_nt(lhs, jnp.concatenate(hot, axis=1))
    placed[...] = acc
    each = 2 * Q_DEV
    for z in range(owners):
        piece = placed[:, z * each : (z + 1) * each]
        wide = jnp.concatenate([piece[0:8], piece[8:16], piece[16:24], jnp.zeros((8, LANES - 3 * each), F32)], axis=1)
        messages[z] = wide.astype(BF16)


def spread_body(arrived, after, copies, joined):
    owners = arrived.shape[0]
    each = 2 * Q_DEV
    for z in range(owners):
        message = arrived[z].astype(F32)
        for g in range(3):
            joined[8 * g : 8 * g + 8, z * each : (z + 1) * each] = message[:, g * each : (g + 1) * each]
    whole = joined[...].astype(BF16)
    for c in range(copies.shape[0]):
        copies[c] = whole


def finish_body(pieces, feat, logit, box, rows):
    owners = pieces.shape[2] // (2 * Q_DEV)
    total = pieces.shape[2]
    chips = pieces.shape[0]
    parts = [
        jnp.concatenate([pieces[c, 0:16, :] for c in range(h * chips // 2, (h + 1) * chips // 2)], axis=0)
        for h in range(2)
    ]
    parts.append(jnp.concatenate([pieces[c, 16:24, :] for c in range(chips)], axis=0))
    images = 2 * owners
    for h in range(3):
        turned = parts[h].astype(F32).T
        for z in range(owners):
            for i in range(2):
                done = 0
                while done < Q_DEV:
                    at = z * 2 * Q_DEV + i * Q_DEV + done
                    n = min(8 - at % 8, Q_DEV - done)
                    rows[h, pl.ds(done * images + 2 * z + i, n, stride=images), :] = turned[at : at + n]
                    done += n
    feat[:, 0:LANES] = rows[0].astype(BF16)
    feat[:, LANES:D] = rows[1].astype(BF16)
    rest = rows[2].astype(BF16)
    logit[...] = rest[:, 0:CLS]
    boxes = rows[2].T[CLS : CLS + KEYS].astype(BF16)
    for r in range(Q_DEV):
        box[r] = boxes[:, r * images : (r + 1) * images]


def token_body(cols_axis, map_w, map_h, image, shard, after, memory, *refs):
    weights, (logit, box) = refs[:12], refs[-2:]
    at = pl.multiple_of(pl.program_id(0) * BLOCK, BLOCK)
    token = at + lax.broadcasted_iota(jnp.int32, (1, BLOCK), 1)
    prior = prior_logits(token, shard[0], map_w, map_h, cols_axis)
    _, logits, boxes = heads(memory[image, pl.ds(at, BLOCK), :], *weights, prior)
    logit[0] = logits
    box[0] = boxes


def token_heads(geometry, image, shard, after, memory, weights, *earlier):
    full = lambda a: pl.BlockSpec(a.shape, lambda j: (0,) * a.ndim)
    return pl.pallas_call(
        lambda *refs: token_body(*geometry, image, *refs),
        out_shape=(
            jax.ShapeDtypeStruct((2, CLS, TOK), BF16),
            jax.ShapeDtypeStruct((2, KEYS, TOK), F32),
        ),
        grid=(TOK // BLOCK,),
        in_specs=[SMEM, VMEM, VMEM] + [full(w) for w in weights[:-1]] + [SMEM] + [ANY] * len(earlier),
        out_specs=(
            pl.BlockSpec((1, CLS, BLOCK), lambda j: (image, 0, j)),
            pl.BlockSpec((1, KEYS, BLOCK), lambda j: (image, 0, j)),
        ),
        input_output_aliases={15: 0, 16: 1} if earlier else {},
        cost_estimate=pl.CostEstimate(flops=2_200_000_000, transcendentals=50_000, bytes_accessed=1_000_000),
        name="token_heads",
    )(shard, after, memory, *weights, *earlier)


def shards(
    memory,
    enc_weight,
    enc_bias,
    norm_gain,
    norm_bias,
    class_weight,
    class_bias,
    box_w1,
    box_b1,
    box_w2,
    box_b2,
    box_w3,
    box_b3,
    picked,
    counts,
):
    owners = lax.axis_size("img")
    cols_axis = lax.axis_size("sx")
    cores = lax.axis_size("sy_1")
    chips = lax.axis_size("sy_0") * cols_axis
    map_w = float(TILE_W * cols_axis)
    map_h = float(TILE_H * lax.axis_size("sy_0") * cores)
    shard = lax.axis_index(PLANE).astype(jnp.int32).reshape(1)
    row = lambda v: v.reshape(1, -1)
    weights = (
        enc_weight,
        row(enc_bias),
        row(norm_gain),
        row(norm_bias),
        class_weight.T,
        row(class_bias),
        box_w1,
        row(box_b1),
        box_w2,
        row(box_b2),
        box_w3.T,
        box_b3,
    )
    geometry = (cols_axis, map_w, map_h)
    memory = near(memory)
    payload = pl.pallas_call(
        lambda *refs: select_body(*geometry, chips, cores, *refs),
        out_shape=pltpu.VMEM((chips * cores, ROWS, LANES), BF16),
        in_specs=[SMEM, SMEM, SMEM] + [VMEM] * 13 + [SMEM],
        out_specs=VMEM,
        scratch_shapes=[pltpu.VMEM((2 * MOST * 16, D), BF16)],
        name="select_rows",
    )(picked, counts.T, shard, picked, memory, *weights)
    received = lax.all_to_all(payload, PLANE, 0, 0, tiled=True)
    tokens = token_heads(geometry, 0, shard, near(payload), memory, weights)
    total = owners * 2 * Q_DEV
    messages = pl.pallas_call(
        lambda *refs: place_body(owners, *refs),
        out_shape=pltpu.VMEM((owners, 8, LANES), BF16),
        in_specs=[VMEM, ANY],
        out_specs=VMEM,
        scratch_shapes=[pltpu.VMEM((ROWS, total), F32)],
        name="place_rows",
    )(near(received), tokens[1])
    arrived = lax.all_to_all(messages, "img", 0, 0, tiled=True)
    token_logits, token_boxes = token_heads(geometry, 1, shard, near(messages), memory, weights, *tokens)
    copies = pl.pallas_call(
        spread_body,
        out_shape=pltpu.VMEM((chips, ROWS, total), BF16),
        in_specs=[VMEM, ANY],
        out_specs=VMEM,
        scratch_shapes=[pltpu.VMEM((ROWS, total), F32)],
        name="spread_rows",
    )(near(arrived), token_boxes)
    pieces = lax.all_to_all(copies, CHIPS, 0, 0, tiled=True)
    feat, logit, box = pl.pallas_call(
        finish_body,
        out_shape=(
            jax.ShapeDtypeStruct((total, D), BF16),
            jax.ShapeDtypeStruct((total, CLS), BF16),
            jax.ShapeDtypeStruct((Q_DEV, KEYS, 2 * owners), BF16),
        ),
        in_specs=[VMEM],
        out_specs=(VMEM, VMEM, VMEM),
        scratch_shapes=[pltpu.VMEM((3, total, LANES), F32)],
        name="finish_rows",
    )(near(pieces))
    owned = lambda a: jnp.transpose(a.reshape(Q_DEV, 2 * owners, -1), (1, 0, 2))
    return (token_logits, token_boxes, owned(feat), owned(logit), jnp.transpose(box, (2, 0, 1)))


def solution(mesh):
    finer = Mesh(
        mesh.devices.reshape(mesh.shape["img"], 4, 2, mesh.shape["sx"]),
        ("img", "sy_0", "sy_1", "sx"),
    )
    in_specs = (
        (P("img", PLANE, None),) + (P(),) * 12 + (P("img", PLANE), P("img", PLANE))
    )
    out_specs = (
        P("img", None, PLANE),
        P("img", None, PLANE),
        P(None, "img", None),
        P(None, "img", None),
        P(None, "img", None),
    )
    return jax.shard_map(
        shards, mesh=finer, in_specs=in_specs, out_specs=out_specs, check_vma=False
    )
```

```python
import jax
import jax.numpy as jnp
from jax import lax
from jax.experimental import pallas as pl
from jax.experimental.pallas import tpu as pltpu
from jax.sharding import Mesh
from jax.sharding import PartitionSpec as P

TILE_H = 40
TILE_W = 64
D = 256
CLS = 91
KEYS = 4
MOST = 40
TOK = 2560
Q_DEV = 20
LANES = 128
ROWS = 24
BLOCK = 640
EARLY = 2
PLANE = ("sy_0", "sy_1", "sx")
CHIPS = ("sy_0", "sx")
F32 = jnp.float32
BF16 = jnp.bfloat16
VMEM = pl.BlockSpec(memory_space=pltpu.VMEM)
SMEM = pl.BlockSpec(memory_space=pltpu.SMEM)
ANY = pl.BlockSpec(memory_space=pl.ANY)
NT = (((1,), (1,)), ((), ()))


def rolled(n, first):
    return [(first + k) % n for k in range(n)]


def plane_order(chips, cores, cols_axis):
    rows_axis = chips // cols_axis
    order = []
    for hi in rolled(rows_axis, rows_axis // 2):
        for core in range(cores):
            for lo in rolled(cols_axis, cols_axis // 2):
                order.append((hi * cores + core) * cols_axis + lo)
    return order


def near(x):
    return pltpu.with_memory_space_constraint(x, pltpu.VMEM)


def dot(a, b):
    return jnp.dot(a, b, preferred_element_type=F32)


def dot_nt(a, b):
    return lax.dot_general(a, b, NT, preferred_element_type=F32)


def column(v):
    n = v.shape[1]
    if n < LANES:
        v = jnp.concatenate([v, jnp.zeros((1, LANES - n), F32)], axis=1)
    return jnp.broadcast_to(v, (LANES, LANES)).T


def heads(x, enc_w, enc_b, gain, bias, cls_t, cls_b, w1, b1, w2, b2, w3_t, b3, prior_logit):
    pre = dot(x, enc_w[...]) + enc_b[...]
    mean = jnp.mean(pre, axis=-1, keepdims=True)
    centered = pre - mean
    var = jnp.mean(centered * centered, axis=-1, keepdims=True)
    out = (centered * lax.rsqrt(var + 1e-05) * gain[...] + bias[...]).astype(BF16)
    n = x.shape[0]
    cls_col = column(cls_b[...])[:CLS]
    if n > LANES:
        cls_col = jnp.concatenate([cls_col] * (n // LANES), axis=1)
    logits = (dot_nt(cls_t[...], out) + cls_col).astype(BF16)
    hidden = jnp.maximum(dot(out, w1[...]) + b1[...], 0.0).astype(BF16)
    hidden = jnp.maximum(dot(hidden, w2[...]) + b2[...], 0.0).astype(BF16)
    which = lax.broadcasted_iota(jnp.int32, (KEYS, n), 0)
    b3_col = jnp.where(which == 0, b3[0], jnp.where(which == 1, b3[1], jnp.where(which == 2, b3[2], b3[3])))
    delta = dot_nt(w3_t[...], hidden) + b3_col
    boxes = jax.nn.sigmoid(delta + prior_logit)
    return out, logits, boxes


def prior_logits(token, shard, map_w, map_h, cols_axis):
    row = shard // cols_axis * TILE_H + (token >> 6)
    col = shard % cols_axis * TILE_W + (token & 63)
    center_x = (col.astype(F32) + 0.5) / map_w
    center_y = (row.astype(F32) + 0.5) / map_h
    n = token.shape[1]
    which = lax.broadcasted_iota(jnp.int32, (4, n), 0)
    prior = jnp.where(which == 0, center_x, jnp.where(which == 1, center_y, 0.05))
    return jnp.log(prior / (1.0 - prior))


def select_body(cols_axis, map_w, map_h, chips, cores, order, picked, counts, shard, pick_vec, memory, *refs):
    weights, (payload, tiles, sem) = refs[:12], refs[12:]
    for i in range(2):
        for k in range(MOST):
            base = pl.multiple_of((picked[i, k] >> 4) << 4, 16)
            j = i * MOST + k
            pltpu.make_async_copy(memory.at[i, pl.ds(base, 16), :], tiles.at[pl.ds(16 * j, 16), :], sem).start()
    n = 2 * MOST * 16
    row = lax.broadcasted_iota(jnp.int32, (LANES, n), 0)
    col = lax.broadcasted_iota(jnp.int32, (LANES, n), 1)
    pick = pick_vec[...]
    pick = jnp.concatenate([pick[0:1], pick[1:2], jnp.zeros((1, LANES - 2 * MOST), jnp.int32)], axis=1)
    pick_col = column((pick & 15).astype(F32)).astype(jnp.int32)
    pick_col = jnp.concatenate([pick_col] * (n // LANES), axis=1)
    chosen = col == row * 16 + pick_col
    chosen = jnp.where(chosen, 1.0, 0.0).astype(BF16)
    prior = prior_logits(pick, shard[0], map_w, map_h, cols_axis)
    pltpu.make_async_copy(memory.at[0, pl.ds(0, n), :], tiles, sem).wait()
    x = dot(chosen, tiles[...]).astype(BF16)
    out, logits, boxes = heads(x, *weights, prior)
    out_t = out.astype(F32).T
    c0 = counts[0, 0].astype(F32)
    c1 = counts[0, 1].astype(F32)

    def marked(v):
        lane = lax.broadcasted_iota(jnp.int32, v.shape, 1)
        return jnp.where(lane == 80, c0, jnp.where(lane == 81, c1, v)).astype(BF16)

    out_t = marked(out_t)
    rest = jnp.concatenate(
        [logits.astype(F32), boxes.astype(F32), jnp.zeros((LANES - CLS - 4, LANES), F32)], axis=0
    )
    rest = marked(rest)
    for hi in range(chips // cols_axis):
        for lo in range(cols_axis):
            c = hi * cols_axis + lo
            for core in range(cores):
                p = (hi * cores + core) * cols_axis + lo
                k = order.index(p)
                payload[k, 0:16, :] = out_t[16 * c : 16 * c + 16, :]
                payload[k, 16:24, :] = rest[8 * c : 8 * c + 8, :]


def place_body(owners, tiles, ring, received, after, messages, placed):
    shards = received.shape[0]
    at = [tiles.index(t) for t in range(shards)]
    flat = jnp.concatenate([received[k] for k in at], axis=0)
    r = lax.broadcasted_iota(jnp.int32, (2 * shards, shards * ROWS), 0)
    m = lax.broadcasted_iota(jnp.int32, (2 * shards, shards * ROWS), 1)
    tile = (m * 2731) >> 16
    wanted = ((r < shards) & (tile == r)) | (tile < r - shards)
    take = jnp.where(wanted & (m == tile * ROWS), 1.0, 0.0)
    res = dot(take.astype(BF16), flat)
    count, start = res[:shards], res[shards:]
    lane = lax.broadcasted_iota(jnp.int32, (shards, LANES), 1)
    image = jnp.where(lane < MOST, 0, 1)
    step = lane - image * MOST
    pick = lambda a: jnp.where(lane < MOST, a[:, 80:81], a[:, 81:82]).astype(jnp.int32)
    slot = pick(start) + step
    valid = (step < pick(count)) & (lane < 2 * MOST)
    owner = (slot * 3277) >> 16
    place = owner * (2 * Q_DEV) + image * Q_DEV + (slot - owner * Q_DEV)
    place = jnp.where(valid, place, -1)
    total = owners * 2 * Q_DEV
    target = lax.broadcasted_iota(jnp.int32, (total, LANES), 0)
    acc = jnp.zeros((ROWS, total), F32)
    for t in range(0, shards, 2):
        hot = [jnp.where(target == place[u : u + 1], 1.0, 0.0).astype(BF16) for u in (t, t + 1)]
        lhs = jnp.concatenate([received[at[t]], received[at[t + 1]]], axis=1)
        acc = acc + dot_nt(lhs, jnp.concatenate(hot, axis=1))
    placed[...] = acc
    each = 2 * Q_DEV
    for z in range(owners):
        piece = placed[:, z * each : (z + 1) * each]
        wide = jnp.concatenate([piece[0:8], piece[8:16], piece[16:24], jnp.zeros((8, LANES - 3 * each), F32)], axis=1)
        messages[ring.index(z)] = wide.astype(BF16)


def spread_body(ring, arrived, after, copies, joined):
    owners = arrived.shape[0]
    each = 2 * Q_DEV
    for z in range(owners):
        message = arrived[ring.index(z)].astype(F32)
        for g in range(3):
            joined[8 * g : 8 * g + 8, z * each : (z + 1) * each] = message[:, g * each : (g + 1) * each]
    whole = joined[...].astype(BF16)
    for c in range(copies.shape[0]):
        copies[c] = whole


def finish_body(pieces, feat, logit, box, rows):
    owners = pieces.shape[2] // (2 * Q_DEV)
    total = pieces.shape[2]
    chips = pieces.shape[0]
    parts = [
        jnp.concatenate([pieces[c, 0:16, :] for c in range(h * chips // 2, (h + 1) * chips // 2)], axis=0)
        for h in range(2)
    ]
    parts.append(jnp.concatenate([pieces[c, 16:24, :] for c in range(chips)], axis=0))
    images = 2 * owners
    for h in range(3):
        turned = parts[h].astype(F32).T
        for z in range(owners):
            for i in range(2):
                done = 0
                while done < Q_DEV:
                    at = z * 2 * Q_DEV + i * Q_DEV + done
                    n = min(8 - at % 8, Q_DEV - done)
                    rows[h, pl.ds(done * images + 2 * z + i, n, stride=images), :] = turned[at : at + n]
                    done += n
    feat[:, 0:LANES] = rows[0].astype(BF16)
    feat[:, LANES:D] = rows[1].astype(BF16)
    rest = rows[2].astype(BF16)
    logit[...] = rest[:, 0:CLS]
    boxes = rows[2].T[CLS : CLS + KEYS].astype(BF16)
    for r in range(Q_DEV):
        box[r] = boxes[:, r * images : (r + 1) * images]


def token_body(cols_axis, map_w, map_h, first, shard, after, memory, *refs):
    weights, (logit, box) = refs[:12], refs[-2:]
    step = first + pl.program_id(0)
    token = step % (TOK // BLOCK) * BLOCK + lax.broadcasted_iota(jnp.int32, (1, BLOCK), 1)
    prior = prior_logits(token, shard[0], map_w, map_h, cols_axis)
    _, logits, boxes = heads(memory[0], *weights, prior)
    logit[0] = logits
    box[0] = boxes


def token_heads(geometry, first, steps, shard, after, memory, weights, *earlier):
    full = lambda a: pl.BlockSpec(a.shape, lambda j: (0,) * a.ndim)
    per = TOK // BLOCK
    return pl.pallas_call(
        lambda *refs: token_body(*geometry, first, *refs),
        out_shape=(
            jax.ShapeDtypeStruct((2, CLS, TOK), BF16),
            jax.ShapeDtypeStruct((2, KEYS, TOK), F32),
        ),
        grid=(steps,),
        in_specs=[SMEM, VMEM, pl.BlockSpec((1, BLOCK, D), lambda j: ((j + first) // per, (j + first) % per, 0))]
        + [full(w) for w in weights[:-1]]
        + [SMEM]
        + [ANY] * len(earlier),
        out_specs=(
            pl.BlockSpec((1, CLS, BLOCK), lambda j: ((j + first) // per, 0, (j + first) % per)),
            pl.BlockSpec((1, KEYS, BLOCK), lambda j: ((j + first) // per, 0, (j + first) % per)),
        ),
        input_output_aliases={15: 0, 16: 1} if earlier else {},
        cost_estimate=pl.CostEstimate(
            flops=450_000_000 * steps, transcendentals=10_000 * steps, bytes_accessed=400_000 * steps
        ),
        name="token_heads",
    )(shard, after, memory, *weights, *earlier)


def shards(
    memory,
    enc_weight,
    enc_bias,
    norm_gain,
    norm_bias,
    class_weight,
    class_bias,
    box_w1,
    box_b1,
    box_w2,
    box_b2,
    box_w3,
    box_b3,
    picked,
    counts,
):
    owners = lax.axis_size("img")
    cols_axis = lax.axis_size("sx")
    cores = lax.axis_size("sy_1")
    chips = lax.axis_size("sy_0") * cols_axis
    map_w = float(TILE_W * cols_axis)
    map_h = float(TILE_H * lax.axis_size("sy_0") * cores)
    shard = lax.axis_index(PLANE).astype(jnp.int32).reshape(1)
    row = lambda v: v.reshape(1, -1)
    weights = (
        enc_weight,
        row(enc_bias),
        row(norm_gain),
        row(norm_bias),
        class_weight.T,
        row(class_bias),
        box_w1,
        row(box_b1),
        box_w2,
        row(box_b2),
        box_w3.T,
        box_b3,
    )
    geometry = (cols_axis, map_w, map_h)
    tiles = plane_order(chips, cores, cols_axis)
    ring = rolled(owners, 3 * owners // 4)
    payload = pl.pallas_call(
        lambda *refs: select_body(*geometry, chips, cores, tiles, *refs),
        out_shape=pltpu.VMEM((chips * cores, ROWS, LANES), BF16),
        in_specs=[SMEM, SMEM, SMEM, VMEM, ANY] + [VMEM] * 11 + [SMEM],
        out_specs=VMEM,
        scratch_shapes=[pltpu.VMEM((2 * MOST * 16, D), BF16), pltpu.SemaphoreType.DMA],
        name="select_rows",
    )(picked, counts.T, shard, picked, memory, *weights)
    received = lax.all_to_all(payload, PLANE, 0, 0, axis_index_groups=[tiles], tiled=True)
    tokens = token_heads(geometry, 0, EARLY, shard, near(payload), memory, weights)
    total = owners * 2 * Q_DEV
    messages = pl.pallas_call(
        lambda *refs: place_body(owners, tiles, ring, *refs),
        out_shape=pltpu.VMEM((owners, 8, LANES), BF16),
        in_specs=[VMEM, ANY],
        out_specs=VMEM,
        scratch_shapes=[pltpu.VMEM((ROWS, total), F32)],
        name="place_rows",
    )(near(received), tokens[1])
    arrived = lax.all_to_all(messages, "img", 0, 0, axis_index_groups=[ring], tiled=True)
    token_logits, token_boxes = token_heads(geometry, EARLY, 2 * TOK // BLOCK - EARLY, shard, near(messages), memory, weights, *tokens)
    copies = pl.pallas_call(
        lambda *refs: spread_body(ring, *refs),
        out_shape=pltpu.VMEM((chips, ROWS, total), BF16),
        in_specs=[VMEM, ANY],
        out_specs=VMEM,
        scratch_shapes=[pltpu.VMEM((ROWS, total), F32)],
        name="spread_rows",
    )(near(arrived), token_boxes)
    pieces = lax.all_to_all(copies, CHIPS, 0, 0, tiled=True)
    feat, logit, box = pl.pallas_call(
        finish_body,
        out_shape=(
            jax.ShapeDtypeStruct((total, D), BF16),
            jax.ShapeDtypeStruct((total, CLS), BF16),
            jax.ShapeDtypeStruct((Q_DEV, KEYS, 2 * owners), BF16),
        ),
        in_specs=[VMEM],
        out_specs=(VMEM, VMEM, VMEM),
        scratch_shapes=[pltpu.VMEM((3, total, LANES), F32)],
        name="finish_rows",
    )(near(pieces))
    owned = lambda a: jnp.transpose(a.reshape(Q_DEV, 2 * owners, -1), (1, 0, 2))
    return (token_logits, token_boxes, owned(feat), owned(logit), jnp.transpose(box, (2, 0, 1)))


def solution(mesh):
    finer = Mesh(
        mesh.devices.reshape(mesh.shape["img"], 4, 2, mesh.shape["sx"]),
        ("img", "sy_0", "sy_1", "sx"),
    )
    in_specs = (
        (P("img", PLANE, None),) + (P(),) * 12 + (P("img", PLANE), P("img", PLANE))
    )
    out_specs = (
        P("img", None, PLANE),
        P("img", None, PLANE),
        P(None, "img", None),
        P(None, "img", None),
        P(None, "img", None),
    )
    return jax.shard_map(
        shards, mesh=finer, in_specs=in_specs, out_specs=out_specs, check_vma=False
    )
```

```python
import jax
import jax.numpy as jnp
from jax import lax
from jax.experimental import pallas as pl
from jax.experimental.pallas import tpu as pltpu
from jax.sharding import Mesh
from jax.sharding import PartitionSpec as P

TILE_H = 40
TILE_W = 64
D = 256
CLS = 91
KEYS = 4
MOST = 40
TOK = 2560
Q_DEV = 20
LANES = 128
HALF = 64
MARK = 120
ROWS = 24
BLOCK = 1280
PLANE = ("sy_0", "sy_1", "sx")
CHIPS = ("sy_0", "sx")
F32 = jnp.float32
BF16 = jnp.bfloat16
VMEM = pl.BlockSpec(memory_space=pltpu.VMEM)
SMEM = pl.BlockSpec(memory_space=pltpu.SMEM)
ANY = pl.BlockSpec(memory_space=pl.ANY)
BIG = (0, 4, 6, 8, 10)
NT = (((1,), (1,)), ((), ()))


def rolled(n, first):
    return [(first + k) % n for k in range(n)]


def plane_order(chips, cores, cols_axis):
    rows_axis = chips // cols_axis
    order = []
    for hi in rolled(rows_axis, rows_axis // 2):
        for core in range(cores):
            for lo in rolled(cols_axis, cols_axis // 2):
                order.append((hi * cores + core) * cols_axis + lo)
    return order


def near(x):
    return pltpu.with_memory_space_constraint(x, pltpu.VMEM)


def dot(a, b):
    return jnp.dot(a, b, preferred_element_type=F32)


def dot_nt(a, b):
    return lax.dot_general(a, b, NT, preferred_element_type=F32)


def column(v):
    n = v.shape[1]
    if n < LANES:
        v = jnp.concatenate([v, jnp.zeros((1, LANES - n), F32)], axis=1)
    return jnp.broadcast_to(v, (LANES, LANES)).T


def heads_split(x, enc_w, enc_b, gain, bias, cls_t, cls_b, w1, b1, w2, b2, w3_t, b3, prior_logit):
    pre = dot(x, enc_w[...]) + enc_b[...]
    mean = jnp.mean(pre, axis=-1, keepdims=True)
    centered = pre - mean
    var = jnp.mean(centered * centered, axis=-1, keepdims=True)
    out = (centered * lax.rsqrt(var + 1e-05) * gain[...] + bias[...]).astype(BF16)
    yield out
    n = x.shape[0]
    cls_col = column(cls_b[...])[:CLS]
    if n > LANES:
        cls_col = jnp.concatenate([cls_col] * (n // LANES), axis=1)
    logits = (dot_nt(cls_t[...], out) + cls_col).astype(BF16)
    hidden = jnp.maximum(dot(out, w1[...]) + b1[...], 0.0).astype(BF16)
    hidden = jnp.maximum(dot(hidden, w2[...]) + b2[...], 0.0).astype(BF16)
    which = lax.broadcasted_iota(jnp.int32, (KEYS, n), 0)
    b3_col = jnp.where(which == 0, b3[0], jnp.where(which == 1, b3[1], jnp.where(which == 2, b3[2], b3[3])))
    delta = dot_nt(w3_t[...], hidden) + b3_col
    boxes = jax.nn.sigmoid(delta + prior_logit)
    yield logits, boxes


def heads(*args):
    out, (logits, boxes) = heads_split(*args)
    return out, logits, boxes


def prior_logits(token, shard, map_w, map_h, cols_axis):
    row = shard // cols_axis * TILE_H + (token >> 6)
    col = shard % cols_axis * TILE_W + (token & 63)
    center_x = (col.astype(F32) + 0.5) / map_w
    center_y = (row.astype(F32) + 0.5) / map_h
    n = token.shape[1]
    which = lax.broadcasted_iota(jnp.int32, (4, n), 0)
    prior = jnp.where(which == 0, center_x, jnp.where(which == 1, center_y, 0.05))
    return jnp.log(prior / (1.0 - prior))


def select_body(cols_axis, map_w, map_h, chips, cores, order, picked, counts, shard, pick_vec, memory, *refs):
    weights, payload, tiles = list(refs[:12]), refs[12], refs[13]
    near_weights, staged, sem, sems = refs[14:-3], refs[-3], refs[-2], refs[-1]
    for i in range(2):
        for k in range(MOST):
            base = pl.multiple_of((picked[i, k] >> 4) << 4, 16)
            j = i * MOST + k
            pltpu.make_async_copy(memory.at[i, pl.ds(base, 16), :], tiles.at[pl.ds(16 * j, 16), :], sem).start()
    loads = [pltpu.make_async_copy(weights[w], near_weights[k], sems.at[k]) for k, w in enumerate(BIG)]
    for load in loads:
        load.start()
    for k, w in enumerate(BIG):
        weights[w] = near_weights[k]
    n = 2 * MOST * 16
    row = lax.broadcasted_iota(jnp.int32, (LANES, n), 0)
    col = lax.broadcasted_iota(jnp.int32, (LANES, n), 1)
    pick = pick_vec[...]
    gap = jnp.zeros((1, HALF - MOST), jnp.int32)
    pick = jnp.concatenate([pick[0:1], gap, pick[1:2], gap], axis=1)
    pick_col = column((pick & 15).astype(F32)).astype(jnp.int32)
    pick_col = jnp.concatenate([pick_col] * (n // LANES), axis=1)
    used = (row & (HALF - 1)) < MOST
    source = jnp.where(row < HALF, row, row - (HALF - MOST)) * 16
    chosen = used & (col == source + pick_col)
    chosen = jnp.where(chosen, 1.0, 0.0).astype(BF16)
    prior = prior_logits(pick, shard[0], map_w, map_h, cols_axis)
    pltpu.make_async_copy(memory.at[0, pl.ds(0, n), :], tiles, sem).wait()
    for load in loads:
        load.wait()
    x = dot(chosen, tiles[...]).astype(BF16)
    c0 = counts[0, 0].astype(F32)
    c1 = counts[0, 1].astype(F32)

    def marked(v):
        lane = lax.broadcasted_iota(jnp.int32, v.shape, 1)
        return jnp.where(lane == MARK, c0, jnp.where(lane == MARK + 1, c1, v)).astype(BF16)

    def stage(rows, at, each):
        for hi in range(chips // cols_axis):
            for lo in range(cols_axis):
                c = hi * cols_axis + lo
                for core in range(cores):
                    k = order.index((hi * cores + core) * cols_axis + lo)
                    staged[k, at : at + each, :] = rows[each * c : each * c + each, :]

    parts = heads_split(x, *weights, prior)
    stage(marked(next(parts).astype(F32).T), 0, 16)
    feats = pltpu.make_async_copy(staged.at[:, 0:16, :], payload.at[:, 0:16, :], sems.at[0])
    feats.start()
    logits, boxes = next(parts)
    rest = [logits.astype(F32), boxes.astype(F32), jnp.zeros((LANES - CLS - KEYS, LANES), F32)]
    stage(marked(jnp.concatenate(rest, axis=0)), 16, 8)
    others = pltpu.make_async_copy(staged.at[:, 16:24, :], payload.at[:, 16:24, :], sems.at[1])
    others.start()
    feats.wait()
    others.wait()


def place_body(owners, tiles, ring, received, after, messages, placed):
    shards = received.shape[0]
    at = [tiles.index(t) for t in range(shards)]
    flat = jnp.concatenate([received[k] for k in at], axis=0)
    r = lax.broadcasted_iota(jnp.int32, (2 * shards, shards * ROWS), 0)
    m = lax.broadcasted_iota(jnp.int32, (2 * shards, shards * ROWS), 1)
    tile = (m * 2731) >> 16
    wanted = ((r < shards) & (tile == r)) | (tile < r - shards)
    take = jnp.where(wanted & (m == tile * ROWS), 1.0, 0.0)
    res = dot(take.astype(BF16), flat)
    count, start = res[:shards], res[shards:]
    lane = lax.broadcasted_iota(jnp.int32, (shards, LANES), 1)
    image = jnp.where(lane < HALF, 0, 1)
    step = lane - image * HALF
    pick = lambda a: jnp.where(lane < HALF, a[:, MARK : MARK + 1], a[:, MARK + 1 : MARK + 2]).astype(jnp.int32)
    slot = pick(start) + step
    valid = (step < pick(count)) & (step < MOST)
    place = jnp.where(valid, slot, -1)
    swapped = pltpu.roll(place, HALF, 1)
    per = owners * Q_DEV
    total = 2 * per
    target = lax.broadcasted_iota(jnp.int32, (per, LANES), 0)
    low = lax.broadcasted_iota(jnp.int32, (1, LANES), 1) < HALF
    low_rows = lax.broadcasted_iota(jnp.int32, (ROWS, LANES), 1) < HALF
    acc = [jnp.zeros((ROWS, per), F32) for _ in range(2)]
    for t in range(0, shards, 4):
        lhs, hot = [[], []], [[], []]
        for u in (t, t + 2):
            a, b = (received[at[v]].astype(F32) for v in (u, u + 1))
            a_swapped, b_swapped = pltpu.roll(a, HALF, 1), pltpu.roll(b, HALF, 1)
            lhs[0].append(jnp.where(low_rows, a, b_swapped).astype(BF16))
            lhs[1].append(jnp.where(low_rows, a_swapped, b).astype(BF16))
            spots = (
                jnp.where(low, place[u : u + 1], swapped[u + 1 : u + 2]),
                jnp.where(low, swapped[u : u + 1], place[u + 1 : u + 2]),
            )
            for i in range(2):
                hot[i].append(jnp.where(target == spots[i], 1.0, 0.0).astype(BF16))
        for i in range(2):
            acc[i] = acc[i] + dot_nt(jnp.concatenate(lhs[i], axis=1), jnp.concatenate(hot[i], axis=1))
    placed[:, 0:per] = acc[0]
    placed[:, per:total] = acc[1]
    each = 2 * Q_DEV
    for z in range(owners):
        spots = (z * Q_DEV, per + z * Q_DEV)
        pieces = [placed[8 * g : 8 * g + 8, at : at + Q_DEV] for g in range(3) for at in spots]
        wide = jnp.concatenate(pieces + [jnp.zeros((8, LANES - 3 * each), F32)], axis=1)
        messages[ring.index(z)] = wide.astype(BF16)


def spread_body(ring, arrived, after, copies, joined):
    owners = arrived.shape[0]
    each = 2 * Q_DEV
    for z in range(owners):
        message = arrived[ring.index(z)].astype(F32)
        for g in range(3):
            joined[8 * g : 8 * g + 8, z * each : (z + 1) * each] = message[:, g * each : (g + 1) * each]
    whole = joined[...].astype(BF16)
    for c in range(copies.shape[0]):
        copies[c] = whole


def finish_body(around, pieces, feat, logit, box, rows):
    owners = pieces.shape[2] // (2 * Q_DEV)
    total = pieces.shape[2]
    chips = pieces.shape[0]
    parts = [
        jnp.concatenate(
            [pieces[around.index(c), 0:16, :] for c in range(h * chips // 2, (h + 1) * chips // 2)], axis=0
        )
        for h in range(2)
    ]
    parts.append(jnp.concatenate([pieces[around.index(c), 16:24, :] for c in range(chips)], axis=0))
    images = 2 * owners
    for h in range(3):
        turned = parts[h].astype(F32).T
        for z in range(owners):
            for i in range(2):
                done = 0
                while done < Q_DEV:
                    at = z * 2 * Q_DEV + i * Q_DEV + done
                    n = min(8 - at % 8, Q_DEV - done)
                    rows[h, pl.ds(done * images + 2 * z + i, n, stride=images), :] = turned[at : at + n]
                    done += n
    feat[:, 0:LANES] = rows[0].astype(BF16)
    feat[:, LANES:D] = rows[1].astype(BF16)
    rest = rows[2].astype(BF16)
    logit[...] = rest[:, 0:CLS]
    boxes = rows[2].T[CLS : CLS + KEYS].astype(BF16)
    for r in range(Q_DEV):
        box[r] = boxes[:, r * images : (r + 1) * images]


def token_body(cols_axis, map_w, map_h, steps, first, last, shard, after, memory, *refs):
    weights, (logit, box, logit_part, box_part, sems) = refs[:12], refs[-5:]
    per = TOK // BLOCK

    def sends(k):
        step = first[0] + k
        image = jnp.where(step >= per, 1, 0)
        at = pl.multiple_of((step - image * per) * BLOCK, BLOCK)
        return (
            pltpu.make_async_copy(logit_part.at[k], logit.at[image, :, pl.ds(at, BLOCK)], sems.at[0, k]),
            pltpu.make_async_copy(box_part.at[k], box.at[image, :, pl.ds(at, BLOCK)], sems.at[1, k]),
        )

    for k in range(steps):

        @pl.when((pl.program_id(0) == k) & (first[0] + k < last[0]))
        def _():
            step = first[0] + k
            local = jnp.where(step >= per, step - per, step)
            token = local * BLOCK + lax.broadcasted_iota(jnp.int32, (1, BLOCK), 1)
            prior = prior_logits(token, shard[0], map_w, map_h, cols_axis)
            _, logits, boxes = heads(memory[0], *weights, prior)
            logit_part[k] = logits
            box_part[k] = boxes
            for send in sends(k):
                send.start()

    @pl.when(pl.program_id(0) == steps - 1)
    def _():
        for k in range(steps):

            @pl.when(first[0] + k < last[0])
            def _():
                for send in sends(k):
                    send.wait()


def token_heads(geometry, first, last, steps, shard, after, memory, weights, *earlier):
    per = TOK // BLOCK

    def rows(j, first, last, shard):
        step = jnp.minimum(first[0] + j, jnp.maximum(last[0] - 1, 0))
        image = jnp.where(step >= per, 1, 0)
        return image, step - image * per, 0

    full = lambda a: pl.BlockSpec(a.shape, lambda j, first, last, shard: (0,) * a.ndim)
    return pl.pallas_call(
        lambda *refs: token_body(*geometry, steps, *refs),
        out_shape=(
            jax.ShapeDtypeStruct((2, CLS, TOK), BF16),
            jax.ShapeDtypeStruct((2, KEYS, TOK), F32),
        ),
        grid_spec=pltpu.PrefetchScalarGridSpec(
            num_scalar_prefetch=3,
            grid=(steps,),
            in_specs=[ANY, pl.BlockSpec((1, BLOCK, D), rows)]
            + [VMEM if k in BIG else full(w) for k, w in enumerate(weights[:-1])]
            + [SMEM]
            + [ANY] * len(earlier),
            out_specs=(ANY, ANY),
            scratch_shapes=[
                pltpu.VMEM((steps, CLS, BLOCK), BF16),
                pltpu.VMEM((steps, KEYS, BLOCK), F32),
                pltpu.SemaphoreType.DMA((2, steps)),
            ],
        ),
        input_output_aliases={17: 0, 18: 1} if earlier else {},
        cost_estimate=pl.CostEstimate(flops=1_300_000_000, transcendentals=30_000, bytes_accessed=1_200_000),
        name="token_heads",
    )(first, last, shard, after, memory, *weights, *earlier)


def shards(
    memory,
    enc_weight,
    enc_bias,
    norm_gain,
    norm_bias,
    class_weight,
    class_bias,
    box_w1,
    box_b1,
    box_w2,
    box_b2,
    box_w3,
    box_b3,
    picked,
    counts,
):
    owners = lax.axis_size("img")
    cols_axis = lax.axis_size("sx")
    cores = lax.axis_size("sy_1")
    chips = lax.axis_size("sy_0") * cols_axis
    map_w = float(TILE_W * cols_axis)
    map_h = float(TILE_H * lax.axis_size("sy_0") * cores)
    shard = lax.axis_index(PLANE).astype(jnp.int32).reshape(1)
    row = lambda v: v.reshape(1, -1)
    weights = (
        enc_weight,
        row(enc_bias),
        row(norm_gain),
        row(norm_bias),
        class_weight.T,
        row(class_bias),
        box_w1,
        row(box_b1),
        box_w2,
        row(box_b2),
        box_w3.T,
        box_b3,
    )
    geometry = (cols_axis, map_w, map_h)
    tiles = plane_order(chips, cores, cols_axis)
    around = plane_order(chips, 1, cols_axis)
    ring = rolled(owners, 5 * owners // 8)
    blocks = 2 * TOK // BLOCK
    ahead = lax.axis_index("img") * 4 < owners
    starts = [(0, 0), (3, 1), (blocks, 3), (blocks, blocks)]
    edges = [jnp.where(ahead, *s).astype(jnp.int32).reshape(1) for s in starts]
    close = tuple(near(w) if k in BIG else w for k, w in enumerate(weights))

    def heads_of(k, after, *earlier):
        steps = max(b - a for a, b in zip(starts[k], starts[k + 1]))
        return token_heads(geometry, edges[k], edges[k + 1], steps, shard, after, memory, close, *earlier)

    payload = pl.pallas_call(
        lambda *refs: select_body(*geometry, chips, cores, tiles, *refs),
        out_shape=jax.ShapeDtypeStruct((chips * cores, ROWS, LANES), BF16),
        in_specs=[SMEM, SMEM, SMEM, VMEM, ANY] + [ANY if w in BIG else VMEM for w in range(11)] + [SMEM],
        out_specs=ANY,
        scratch_shapes=[pltpu.VMEM((2 * MOST * 16, D), BF16)]
        + [pltpu.VMEM(weights[w].shape, BF16) for w in BIG]
        + [pltpu.VMEM((chips * cores, ROWS, LANES), BF16)]
        + [pltpu.SemaphoreType.DMA, pltpu.SemaphoreType.DMA((len(BIG),))],
        name="select_rows",
    )(picked, counts.T, shard, picked, memory, *weights)
    received = lax.all_to_all(payload, PLANE, 0, 0, axis_index_groups=[tiles], tiled=True)
    tokens = heads_of(0, payload)
    total = owners * 2 * Q_DEV
    messages = pl.pallas_call(
        lambda *refs: place_body(owners, tiles, ring, *refs),
        out_shape=pltpu.VMEM((owners, 8, LANES), BF16),
        in_specs=[VMEM, ANY],
        out_specs=VMEM,
        scratch_shapes=[pltpu.VMEM((ROWS, total), F32)],
        name="place_rows",
    )(near(received), tokens[1])
    arrived = lax.all_to_all(messages, "img", 0, 0, axis_index_groups=[ring], tiled=True)
    tokens = heads_of(1, messages, *tokens)
    copies = pl.pallas_call(
        lambda *refs: spread_body(ring, *refs),
        out_shape=pltpu.VMEM((chips, ROWS, total), BF16),
        in_specs=[VMEM, ANY],
        out_specs=VMEM,
        scratch_shapes=[pltpu.VMEM((ROWS, total), F32)],
        name="spread_rows",
    )(near(arrived), tokens[1])
    pieces = lax.all_to_all(copies, CHIPS, 0, 0, axis_index_groups=[around], tiled=True)
    token_logits, token_boxes = heads_of(2, copies, *tokens)
    feat, logit, box = pl.pallas_call(
        lambda *refs: finish_body(around, *refs),
        out_shape=(
            jax.ShapeDtypeStruct((total, D), BF16),
            jax.ShapeDtypeStruct((total, CLS), BF16),
            jax.ShapeDtypeStruct((Q_DEV, KEYS, 2 * owners), BF16),
        ),
        in_specs=[VMEM],
        out_specs=(VMEM, VMEM, VMEM),
        scratch_shapes=[pltpu.VMEM((3, total, LANES), F32)],
        name="finish_rows",
    )(near(pieces))
    owned = lambda a: jnp.transpose(a.reshape(Q_DEV, 2 * owners, -1), (1, 0, 2))
    return (token_logits, token_boxes, owned(feat), owned(logit), jnp.transpose(box, (2, 0, 1)))


def solution(mesh):
    finer = Mesh(
        mesh.devices.reshape(mesh.shape["img"], 4, 2, mesh.shape["sx"]),
        ("img", "sy_0", "sy_1", "sx"),
    )
    in_specs = (
        (P("img", PLANE, None),) + (P(),) * 12 + (P("img", PLANE), P("img", PLANE))
    )
    out_specs = (
        P("img", None, PLANE),
        P("img", None, PLANE),
        P(None, "img", None),
        P(None, "img", None),
        P(None, "img", None),
    )
    return jax.shard_map(
        shards, mesh=finer, in_specs=in_specs, out_specs=out_specs, check_vma=False
    )
```

```python
import jax
import jax.numpy as jnp
from jax import lax
from jax.experimental import pallas as pl
from jax.experimental.pallas import tpu as pltpu
from jax.sharding import Mesh
from jax.sharding import PartitionSpec as P

TILE_H = 40
TILE_W = 64
D = 256
CLS = 91
KEYS = 4
MOST = 40
TOK = 2560
Q_DEV = 20
LANES = 128
HALF = 64
MARK = 120
ROWS = 24
BLOCK = 1280
PLANE = ("sy_0", "sy_1", "sx")
CHIPS = ("sy_0", "sx")
F32 = jnp.float32
BF16 = jnp.bfloat16
VMEM = pl.BlockSpec(memory_space=pltpu.VMEM)
SMEM = pl.BlockSpec(memory_space=pltpu.SMEM)
ANY = pl.BlockSpec(memory_space=pl.ANY)
BIG = (0, 4, 6, 8, 10)
NT = (((1,), (1,)), ((), ()))


def rolled(n, first):
    return [(first + k) % n for k in range(n)]


def plane_order(chips, cores, cols_axis):
    rows_axis = chips // cols_axis
    order = []
    for hi in rolled(rows_axis, rows_axis // 2):
        for core in range(cores):
            for lo in rolled(cols_axis, cols_axis // 2):
                order.append((hi * cores + core) * cols_axis + lo)
    return order


def near(x):
    return pltpu.with_memory_space_constraint(x, pltpu.VMEM)


def dot(a, b):
    return jnp.dot(a, b, preferred_element_type=F32)


def dot_nt(a, b):
    return lax.dot_general(a, b, NT, preferred_element_type=F32)


def column(v):
    n = v.shape[1]
    if n < LANES:
        v = jnp.concatenate([v, jnp.zeros((1, LANES - n), F32)], axis=1)
    return jnp.broadcast_to(v, (LANES, LANES)).T


def heads_split(x, enc_w, enc_b, gain, bias, cls_t, cls_b, w1, b1, w2, b2, w3_t, b3, prior_logit):
    pre = dot(x, enc_w[...]) + enc_b[...]
    mean = jnp.mean(pre, axis=-1, keepdims=True)
    centered = pre - mean
    var = jnp.mean(centered * centered, axis=-1, keepdims=True)
    out = (centered * lax.rsqrt(var + 1e-05) * gain[...] + bias[...]).astype(BF16)
    yield out
    n = x.shape[0]
    cls_col = column(cls_b[...])[:CLS]
    if n > LANES:
        cls_col = jnp.concatenate([cls_col] * (n // LANES), axis=1)
    logits = (dot_nt(cls_t[...], out) + cls_col).astype(BF16)
    hidden = jnp.maximum(dot(out, w1[...]) + b1[...], 0.0).astype(BF16)
    hidden = jnp.maximum(dot(hidden, w2[...]) + b2[...], 0.0).astype(BF16)
    which = lax.broadcasted_iota(jnp.int32, (KEYS, n), 0)
    b3_col = jnp.where(which == 0, b3[0], jnp.where(which == 1, b3[1], jnp.where(which == 2, b3[2], b3[3])))
    delta = dot_nt(w3_t[...], hidden) + b3_col
    boxes = jax.nn.sigmoid(delta + prior_logit)
    yield logits, boxes


def heads(*args):
    out, (logits, boxes) = heads_split(*args)
    return out, logits, boxes


def prior_logits(token, shard, map_w, map_h, cols_axis):
    row = shard // cols_axis * TILE_H + (token >> 6)
    col = shard % cols_axis * TILE_W + (token & 63)
    center_x = (col.astype(F32) + 0.5) / map_w
    center_y = (row.astype(F32) + 0.5) / map_h
    n = token.shape[1]
    which = lax.broadcasted_iota(jnp.int32, (4, n), 0)
    prior = jnp.where(which == 0, center_x, jnp.where(which == 1, center_y, 0.05))
    return jnp.log(prior / (1.0 - prior))


def select_body(cols_axis, map_w, map_h, chips, cores, order, picked, counts, shard, pick_vec, memory, *refs):
    weights, payload, tiles = list(refs[:12]), refs[12], refs[13]
    near_weights, staged, sem, sems = refs[14:-3], refs[-3], refs[-2], refs[-1]
    for i in range(2):
        for k in range(MOST):
            base = pl.multiple_of((picked[i, k] >> 4) << 4, 16)
            j = i * MOST + k
            pltpu.make_async_copy(memory.at[i, pl.ds(base, 16), :], tiles.at[pl.ds(16 * j, 16), :], sem).start()
    loads = [pltpu.make_async_copy(weights[w], near_weights[k], sems.at[k]) for k, w in enumerate(BIG)]
    for load in loads:
        load.start()
    for k, w in enumerate(BIG):
        weights[w] = near_weights[k]
    n = 2 * MOST * 16
    row = lax.broadcasted_iota(jnp.int32, (LANES, n), 0)
    col = lax.broadcasted_iota(jnp.int32, (LANES, n), 1)
    pick = pick_vec[...]
    gap = jnp.zeros((1, HALF - MOST), jnp.int32)
    pick = jnp.concatenate([pick[0:1], gap, pick[1:2], gap], axis=1)
    pick_col = column((pick & 15).astype(F32)).astype(jnp.int32)
    pick_col = jnp.concatenate([pick_col] * (n // LANES), axis=1)
    used = (row & (HALF - 1)) < MOST
    source = jnp.where(row < HALF, row, row - (HALF - MOST)) * 16
    chosen = used & (col == source + pick_col)
    chosen = jnp.where(chosen, 1.0, 0.0).astype(BF16)
    prior = prior_logits(pick, shard[0], map_w, map_h, cols_axis)
    pltpu.make_async_copy(memory.at[0, pl.ds(0, n), :], tiles, sem).wait()
    for load in loads:
        load.wait()
    x = dot(chosen, tiles[...]).astype(BF16)
    c0 = counts[0, 0].astype(F32)
    c1 = counts[0, 1].astype(F32)

    def marked(v):
        lane = lax.broadcasted_iota(jnp.int32, v.shape, 1)
        return jnp.where(lane == MARK, c0, jnp.where(lane == MARK + 1, c1, v)).astype(BF16)

    def stage(rows, at, each):
        for hi in range(chips // cols_axis):
            for lo in range(cols_axis):
                c = hi * cols_axis + lo
                for core in range(cores):
                    k = order.index((hi * cores + core) * cols_axis + lo)
                    staged[k, at : at + each, :] = rows[each * c : each * c + each, :]

    parts = heads_split(x, *weights, prior)
    stage(marked(next(parts).astype(F32).T), 0, 16)
    feats = pltpu.make_async_copy(staged.at[:, 0:16, :], payload.at[:, 0:16, :], sems.at[0])
    feats.start()
    logits, boxes = next(parts)
    rest = [logits.astype(F32), boxes.astype(F32), jnp.zeros((LANES - CLS - KEYS, LANES), F32)]
    stage(marked(jnp.concatenate(rest, axis=0)), 16, 8)
    others = pltpu.make_async_copy(staged.at[:, 16:24, :], payload.at[:, 16:24, :], sems.at[1])
    others.start()
    feats.wait()
    others.wait()


def place_body(owners, tiles, ring, received, after, messages, placed):
    shards = received.shape[0]
    at = [tiles.index(t) for t in range(shards)]
    flat = jnp.concatenate([received[k] for k in at], axis=0)
    r = lax.broadcasted_iota(jnp.int32, (2 * shards, shards * ROWS), 0)
    m = lax.broadcasted_iota(jnp.int32, (2 * shards, shards * ROWS), 1)
    tile = (m * 2731) >> 16
    wanted = ((r < shards) & (tile == r)) | (tile < r - shards)
    take = jnp.where(wanted & (m == tile * ROWS), 1.0, 0.0)
    res = dot(take.astype(BF16), flat)
    count, start = res[:shards], res[shards:]
    lane = lax.broadcasted_iota(jnp.int32, (shards, LANES), 1)
    image = jnp.where(lane < HALF, 0, 1)
    step = lane - image * HALF
    pick = lambda a: jnp.where(lane < HALF, a[:, MARK : MARK + 1], a[:, MARK + 1 : MARK + 2]).astype(jnp.int32)
    slot = pick(start) + step
    valid = (step < pick(count)) & (step < MOST)
    place = jnp.where(valid, slot, -1)
    swapped = pltpu.roll(place, HALF, 1)
    per = owners * Q_DEV
    total = 2 * per
    target = lax.broadcasted_iota(jnp.int32, (per, LANES), 0)
    low = lax.broadcasted_iota(jnp.int32, (1, LANES), 1) < HALF
    low_rows = lax.broadcasted_iota(jnp.int32, (ROWS, LANES), 1) < HALF
    acc = [jnp.zeros((ROWS, per), F32) for _ in range(2)]
    for t in range(0, shards, 4):
        lhs, hot = [[], []], [[], []]
        for u in (t, t + 2):
            a, b = (received[at[v]].astype(F32) for v in (u, u + 1))
            a_swapped, b_swapped = pltpu.roll(a, HALF, 1), pltpu.roll(b, HALF, 1)
            lhs[0].append(jnp.where(low_rows, a, b_swapped).astype(BF16))
            lhs[1].append(jnp.where(low_rows, a_swapped, b).astype(BF16))
            spots = (
                jnp.where(low, place[u : u + 1], swapped[u + 1 : u + 2]),
                jnp.where(low, swapped[u : u + 1], place[u + 1 : u + 2]),
            )
            for i in range(2):
                hot[i].append(jnp.where(target == spots[i], 1.0, 0.0).astype(BF16))
        for i in range(2):
            acc[i] = acc[i] + dot_nt(jnp.concatenate(lhs[i], axis=1), jnp.concatenate(hot[i], axis=1))
    placed[:, 0:per] = acc[0]
    placed[:, per:total] = acc[1]
    each = 2 * Q_DEV
    for z in range(owners):
        spots = (z * Q_DEV, per + z * Q_DEV)
        pieces = [placed[8 * g : 8 * g + 8, at : at + Q_DEV] for g in range(3) for at in spots]
        wide = jnp.concatenate(pieces + [jnp.zeros((8, LANES - 3 * each), F32)], axis=1)
        messages[ring.index(z)] = wide.astype(BF16)


def spread_body(ring, arrived, copies, joined):
    owners = arrived.shape[0]
    each = 2 * Q_DEV
    for z in range(owners):
        message = arrived[ring.index(z)].astype(F32)
        for g in range(3):
            joined[8 * g : 8 * g + 8, z * each : (z + 1) * each] = message[:, g * each : (g + 1) * each]
    whole = joined[...].astype(BF16)
    for c in range(copies.shape[0]):
        copies[c] = whole


def finish_body(around, pieces, feat, logit, box, rows):
    owners = pieces.shape[2] // (2 * Q_DEV)
    total = pieces.shape[2]
    chips = pieces.shape[0]
    parts = [
        jnp.concatenate(
            [pieces[around.index(c), 0:16, :] for c in range(h * chips // 2, (h + 1) * chips // 2)], axis=0
        )
        for h in range(2)
    ]
    parts.append(jnp.concatenate([pieces[around.index(c), 16:24, :] for c in range(chips)], axis=0))
    images = 2 * owners

    def reorder(h):
        turned = parts[h].astype(F32).T
        for z in range(owners):
            for i in range(2):
                done = 0
                while done < Q_DEV:
                    at = z * 2 * Q_DEV + i * Q_DEV + done
                    n = min(8 - at % 8, Q_DEV - done)
                    rows[h, pl.ds(done * images + 2 * z + i, n, stride=images), :] = turned[at : at + n]
                    done += n

    reorder(2)
    rest = rows[2].astype(BF16)
    logit[...] = rest[:, 0:CLS]
    boxes = rows[2].T[CLS : CLS + KEYS].astype(BF16)
    for r in range(Q_DEV):
        box[r] = boxes[:, r * images : (r + 1) * images]
    for h in range(2):
        reorder(h)
        feat[:, h * LANES : (h + 1) * LANES] = rows[h].astype(BF16)


def token_body(cols_axis, map_w, map_h, steps, first, last, shard, after, memory, *refs):
    weights, (logit, box, logit_part, box_part, sems) = refs[:12], refs[-5:]
    per = TOK // BLOCK

    def sends(k):
        step = first[0] + k
        image = jnp.where(step >= per, 1, 0)
        at = pl.multiple_of((step - image * per) * BLOCK, BLOCK)
        return (
            pltpu.make_async_copy(logit_part.at[k], logit.at[image, :, pl.ds(at, BLOCK)], sems.at[0, k]),
            pltpu.make_async_copy(box_part.at[k], box.at[image, :, pl.ds(at, BLOCK)], sems.at[1, k]),
        )

    for k in range(steps):

        @pl.when((pl.program_id(0) == k) & (first[0] + k < last[0]))
        def _():
            step = first[0] + k
            local = jnp.where(step >= per, step - per, step)
            token = local * BLOCK + lax.broadcasted_iota(jnp.int32, (1, BLOCK), 1)
            prior = prior_logits(token, shard[0], map_w, map_h, cols_axis)
            _, logits, boxes = heads(memory[0], *weights, prior)
            logit_part[k] = logits
            box_part[k] = boxes
            for send in sends(k):
                send.start()

    @pl.when(pl.program_id(0) == steps - 1)
    def _():
        for k in range(steps):

            @pl.when(first[0] + k < last[0])
            def _():
                for send in sends(k):
                    send.wait()


def token_heads(geometry, first, last, steps, shard, after, memory, weights, *earlier):
    per = TOK // BLOCK

    def rows(j, first, last, shard):
        step = jnp.minimum(first[0] + j, jnp.maximum(last[0] - 1, 0))
        image = jnp.where(step >= per, 1, 0)
        return image, step - image * per, 0

    full = lambda a: pl.BlockSpec(a.shape, lambda j, first, last, shard: (0,) * a.ndim)
    return pl.pallas_call(
        lambda *refs: token_body(*geometry, steps, *refs),
        out_shape=(
            jax.ShapeDtypeStruct((2, CLS, TOK), BF16),
            jax.ShapeDtypeStruct((2, KEYS, TOK), F32),
        ),
        grid_spec=pltpu.PrefetchScalarGridSpec(
            num_scalar_prefetch=3,
            grid=(steps,),
            in_specs=[ANY, pl.BlockSpec((1, BLOCK, D), rows)]
            + [VMEM if k in BIG else full(w) for k, w in enumerate(weights[:-1])]
            + [SMEM]
            + [ANY] * len(earlier),
            out_specs=(ANY, ANY),
            scratch_shapes=[
                pltpu.VMEM((steps, CLS, BLOCK), BF16),
                pltpu.VMEM((steps, KEYS, BLOCK), F32),
                pltpu.SemaphoreType.DMA((2, steps)),
            ],
        ),
        input_output_aliases={17: 0, 18: 1} if earlier else {},
        cost_estimate=pl.CostEstimate(flops=1_300_000_000, transcendentals=30_000, bytes_accessed=1_200_000),
        name="token_heads",
    )(first, last, shard, after, memory, *weights, *earlier)


def shards(
    memory,
    enc_weight,
    enc_bias,
    norm_gain,
    norm_bias,
    class_weight,
    class_bias,
    box_w1,
    box_b1,
    box_w2,
    box_b2,
    box_w3,
    box_b3,
    picked,
    counts,
):
    owners = lax.axis_size("img")
    cols_axis = lax.axis_size("sx")
    cores = lax.axis_size("sy_1")
    chips = lax.axis_size("sy_0") * cols_axis
    map_w = float(TILE_W * cols_axis)
    map_h = float(TILE_H * lax.axis_size("sy_0") * cores)
    shard = lax.axis_index(PLANE).astype(jnp.int32).reshape(1)
    row = lambda v: v.reshape(1, -1)
    weights = (
        enc_weight,
        row(enc_bias),
        row(norm_gain),
        row(norm_bias),
        class_weight.T,
        row(class_bias),
        box_w1,
        row(box_b1),
        box_w2,
        row(box_b2),
        box_w3.T,
        box_b3,
    )
    geometry = (cols_axis, map_w, map_h)
    tiles = plane_order(chips, cores, cols_axis)
    around = plane_order(chips, 1, cols_axis)
    ring = rolled(owners, 5 * owners // 8)
    blocks = 2 * TOK // BLOCK
    quarter = lax.axis_index("img") * 4 // owners
    starts = [(0, 0), (blocks, blocks // 2), (blocks, blocks)]
    middle = jnp.where(quarter == 0, blocks, jnp.where(quarter == 1, blocks * 3 // 4, blocks // 2))
    edges = [jnp.asarray(e, jnp.int32).reshape(1) for e in (0, middle, blocks)]
    close = tuple(near(w) if k in BIG else w for k, w in enumerate(weights))

    def heads_of(k, after, *earlier):
        steps = max(b - a for a, b in zip(starts[k], starts[k + 1]))
        return token_heads(geometry, edges[k], edges[k + 1], steps, shard, after, memory, close, *earlier)

    payload = pl.pallas_call(
        lambda *refs: select_body(*geometry, chips, cores, tiles, *refs),
        out_shape=jax.ShapeDtypeStruct((chips * cores, ROWS, LANES), BF16),
        in_specs=[SMEM, SMEM, SMEM, VMEM, ANY] + [ANY if w in BIG else VMEM for w in range(11)] + [SMEM],
        out_specs=ANY,
        scratch_shapes=[pltpu.VMEM((2 * MOST * 16, D), BF16)]
        + [pltpu.VMEM(weights[w].shape, BF16) for w in BIG]
        + [pltpu.VMEM((chips * cores, ROWS, LANES), BF16)]
        + [pltpu.SemaphoreType.DMA, pltpu.SemaphoreType.DMA((len(BIG),))],
        name="select_rows",
    )(picked, counts.T, shard, picked, memory, *weights)
    received = lax.all_to_all(payload, PLANE, 0, 0, axis_index_groups=[tiles], tiled=True)
    tokens = heads_of(0, payload)
    total = owners * 2 * Q_DEV
    messages = pl.pallas_call(
        lambda *refs: place_body(owners, tiles, ring, *refs),
        out_shape=pltpu.VMEM((owners, 8, LANES), BF16),
        in_specs=[VMEM, ANY],
        out_specs=VMEM,
        scratch_shapes=[pltpu.VMEM((ROWS, total), F32)],
        name="place_rows",
    )(near(received), tokens[1])
    arrived = lax.all_to_all(messages, "img", 0, 0, axis_index_groups=[ring], tiled=True)
    copies = pl.pallas_call(
        lambda *refs: spread_body(ring, *refs),
        out_shape=pltpu.VMEM((chips, ROWS, total), BF16),
        in_specs=[VMEM],
        out_specs=VMEM,
        scratch_shapes=[pltpu.VMEM((ROWS, total), F32)],
        name="spread_rows",
    )(near(arrived))
    pieces = lax.all_to_all(copies, CHIPS, 0, 0, axis_index_groups=[around], tiled=True)
    token_logits, token_boxes = heads_of(1, copies, *tokens)
    feat, logit, box = pl.pallas_call(
        lambda *refs: finish_body(around, *refs),
        out_shape=(
            jax.ShapeDtypeStruct((total, D), BF16),
            jax.ShapeDtypeStruct((total, CLS), BF16),
            jax.ShapeDtypeStruct((Q_DEV, KEYS, 2 * owners), BF16),
        ),
        in_specs=[VMEM],
        out_specs=(VMEM, VMEM, VMEM),
        scratch_shapes=[pltpu.VMEM((3, total, LANES), F32)],
        name="finish_rows",
    )(near(pieces))
    owned = lambda a: jnp.transpose(a.reshape(Q_DEV, 2 * owners, -1), (1, 0, 2))
    return (token_logits, token_boxes, owned(feat), owned(logit), jnp.transpose(box, (2, 0, 1)))


def solution(mesh):
    finer = Mesh(
        mesh.devices.reshape(mesh.shape["img"], 4, 2, mesh.shape["sx"]),
        ("img", "sy_0", "sy_1", "sx"),
    )
    in_specs = (
        (P("img", PLANE, None),) + (P(),) * 12 + (P("img", PLANE), P("img", PLANE))
    )
    out_specs = (
        P("img", None, PLANE),
        P("img", None, PLANE),
        P(None, "img", None),
        P(None, "img", None),
        P(None, "img", None),
    )
    return jax.shard_map(
        shards, mesh=finer, in_specs=in_specs, out_specs=out_specs, check_vma=False
    )
```

```python
import jax
import jax.numpy as jnp
from jax import lax
from jax.experimental import pallas as pl
from jax.experimental.pallas import tpu as pltpu
from jax.sharding import Mesh
from jax.sharding import PartitionSpec as P

TILE_H = 40
TILE_W = 64
D = 256
CLS = 91
KEYS = 4
MOST = 40
TOK = 2560
Q_DEV = 20
LANES = 128
HALF = 64
MARK = 120
ROWS = 24
BLOCK = 1280
PLANE = ("sy_0", "sy_1", "sx")
CHIPS = ("sy_0", "sx")
F32 = jnp.float32
BF16 = jnp.bfloat16
VMEM = pl.BlockSpec(memory_space=pltpu.VMEM)
SMEM = pl.BlockSpec(memory_space=pltpu.SMEM)
ANY = pl.BlockSpec(memory_space=pl.ANY)
BIG = (0, 4, 6, 8, 10)
NT = (((1,), (1,)), ((), ()))


def rolled(n, first):
    return [(first + k) % n for k in range(n)]


def plane_order(chips, cores, cols_axis):
    rows_axis = chips // cols_axis
    order = []
    for hi in rolled(rows_axis, rows_axis // 2):
        for core in range(cores):
            for lo in rolled(cols_axis, cols_axis // 2):
                order.append((hi * cores + core) * cols_axis + lo)
    return order


def near(x):
    return pltpu.with_memory_space_constraint(x, pltpu.VMEM)


def dot(a, b):
    return jnp.dot(a, b, preferred_element_type=F32)


def dot_nt(a, b):
    return lax.dot_general(a, b, NT, preferred_element_type=F32)


def column(v):
    n = v.shape[1]
    if n < LANES:
        v = jnp.concatenate([v, jnp.zeros((1, LANES - n), F32)], axis=1)
    return jnp.broadcast_to(v, (LANES, LANES)).T


def heads_split(x, enc_w, enc_b, gain, bias, cls_t, cls_b, w1, b1, w2, b2, w3_t, b3, prior_logit):
    pre = dot(x, enc_w[...]) + enc_b[...]
    mean = jnp.mean(pre, axis=-1, keepdims=True)
    centered = pre - mean
    var = jnp.mean(centered * centered, axis=-1, keepdims=True)
    out = (centered * lax.rsqrt(var + 1e-05) * gain[...] + bias[...]).astype(BF16)
    yield out
    n = x.shape[0]
    cls_col = column(cls_b[...])[:CLS]
    if n > LANES:
        cls_col = jnp.concatenate([cls_col] * (n // LANES), axis=1)
    logits = (dot_nt(cls_t[...], out) + cls_col).astype(BF16)
    hidden = jnp.maximum(dot(out, w1[...]) + b1[...], 0.0).astype(BF16)
    hidden = jnp.maximum(dot(hidden, w2[...]) + b2[...], 0.0).astype(BF16)
    which = lax.broadcasted_iota(jnp.int32, (KEYS, n), 0)
    b3_col = jnp.where(which == 0, b3[0], jnp.where(which == 1, b3[1], jnp.where(which == 2, b3[2], b3[3])))
    delta = dot_nt(w3_t[...], hidden) + b3_col
    boxes = jax.nn.sigmoid(delta + prior_logit)
    yield logits, boxes


def heads(*args):
    out, (logits, boxes) = heads_split(*args)
    return out, logits, boxes


def prior_logits(token, shard, map_w, map_h, cols_axis):
    row = shard // cols_axis * TILE_H + (token >> 6)
    col = shard % cols_axis * TILE_W + (token & 63)
    center_x = (col.astype(F32) + 0.5) / map_w
    center_y = (row.astype(F32) + 0.5) / map_h
    n = token.shape[1]
    which = lax.broadcasted_iota(jnp.int32, (4, n), 0)
    prior = jnp.where(which == 0, center_x, jnp.where(which == 1, center_y, 0.05))
    return jnp.log(prior / (1.0 - prior))


def select_body(cols_axis, map_w, map_h, chips, cores, order, picked, counts, shard, pick_vec, memory, *refs):
    weights, payload, tiles = list(refs[:12]), refs[12], refs[13]
    near_weights, staged, sem, sems = refs[14:-3], refs[-3], refs[-2], refs[-1]
    for i in range(2):
        for k in range(MOST):
            base = pl.multiple_of((picked[i, k] >> 4) << 4, 16)
            j = i * MOST + k
            pltpu.make_async_copy(memory.at[i, pl.ds(base, 16), :], tiles.at[pl.ds(16 * j, 16), :], sem).start()
    loads = [pltpu.make_async_copy(weights[w], near_weights[k], sems.at[k]) for k, w in enumerate(BIG)]
    for load in loads:
        load.start()
    for k, w in enumerate(BIG):
        weights[w] = near_weights[k]
    n = 2 * MOST * 16
    row = lax.broadcasted_iota(jnp.int32, (LANES, n), 0)
    col = lax.broadcasted_iota(jnp.int32, (LANES, n), 1)
    pick = pick_vec[...]
    gap = jnp.zeros((1, HALF - MOST), jnp.int32)
    pick = jnp.concatenate([pick[0:1], gap, pick[1:2], gap], axis=1)
    pick_col = column((pick & 15).astype(F32)).astype(jnp.int32)
    pick_col = jnp.concatenate([pick_col] * (n // LANES), axis=1)
    used = (row & (HALF - 1)) < MOST
    source = jnp.where(row < HALF, row, row - (HALF - MOST)) * 16
    chosen = used & (col == source + pick_col)
    chosen = jnp.where(chosen, 1.0, 0.0).astype(BF16)
    prior = prior_logits(pick, shard[0], map_w, map_h, cols_axis)
    pltpu.make_async_copy(memory.at[0, pl.ds(0, n), :], tiles, sem).wait()
    for load in loads:
        load.wait()
    x = dot(chosen, tiles[...]).astype(BF16)
    c0 = counts[0, 0].astype(F32)
    c1 = counts[0, 1].astype(F32)

    def marked(v):
        lane = lax.broadcasted_iota(jnp.int32, v.shape, 1)
        return jnp.where(lane == MARK, c0, jnp.where(lane == MARK + 1, c1, v)).astype(BF16)

    def stage(rows, at, each):
        for hi in range(chips // cols_axis):
            for lo in range(cols_axis):
                c = hi * cols_axis + lo
                for core in range(cores):
                    k = order.index((hi * cores + core) * cols_axis + lo)
                    staged[k, at : at + each, :] = rows[each * c : each * c + each, :]

    parts = heads_split(x, *weights, prior)
    stage(marked(next(parts).astype(F32).T), 0, 16)
    feats = pltpu.make_async_copy(staged.at[:, 0:16, :], payload.at[:, 0:16, :], sems.at[0])
    feats.start()
    logits, boxes = next(parts)
    rest = [logits.astype(F32), boxes.astype(F32), jnp.zeros((LANES - CLS - KEYS, LANES), F32)]
    stage(marked(jnp.concatenate(rest, axis=0)), 16, 8)
    others = pltpu.make_async_copy(staged.at[:, 16:24, :], payload.at[:, 16:24, :], sems.at[1])
    others.start()
    feats.wait()
    others.wait()


def place_body(owners, tiles, ring, received, after, messages, placed):
    shards = received.shape[0]
    at = [tiles.index(t) for t in range(shards)]
    flat = jnp.concatenate([received[k] for k in at], axis=0)
    r = lax.broadcasted_iota(jnp.int32, (2 * shards, shards * ROWS), 0)
    m = lax.broadcasted_iota(jnp.int32, (2 * shards, shards * ROWS), 1)
    tile = (m * 2731) >> 16
    wanted = ((r < shards) & (tile == r)) | (tile < r - shards)
    take = jnp.where(wanted & (m == tile * ROWS), 1.0, 0.0)
    res = dot(take.astype(BF16), flat)
    count, start = res[:shards], res[shards:]
    lane = lax.broadcasted_iota(jnp.int32, (shards, LANES), 1)
    image = jnp.where(lane < HALF, 0, 1)
    step = lane - image * HALF
    pick = lambda a: jnp.where(lane < HALF, a[:, MARK : MARK + 1], a[:, MARK + 1 : MARK + 2]).astype(jnp.int32)
    slot = pick(start) + step
    valid = (step < pick(count)) & (step < MOST)
    place = jnp.where(valid, slot, -1)
    swapped = pltpu.roll(place, HALF, 1)
    per = owners * Q_DEV
    total = 2 * per
    target = lax.broadcasted_iota(jnp.int32, (per, LANES), 0)
    low = lax.broadcasted_iota(jnp.int32, (1, LANES), 1) < HALF
    low_rows = lax.broadcasted_iota(jnp.int32, (ROWS, LANES), 1) < HALF
    acc = [jnp.zeros((ROWS, per), F32) for _ in range(2)]
    for t in range(0, shards, 4):
        lhs, hot = [[], []], [[], []]
        for u in (t, t + 2):
            a, b = (received[at[v]].astype(F32) for v in (u, u + 1))
            a_swapped, b_swapped = pltpu.roll(a, HALF, 1), pltpu.roll(b, HALF, 1)
            lhs[0].append(jnp.where(low_rows, a, b_swapped).astype(BF16))
            lhs[1].append(jnp.where(low_rows, a_swapped, b).astype(BF16))
            spots = (
                jnp.where(low, place[u : u + 1], swapped[u + 1 : u + 2]),
                jnp.where(low, swapped[u : u + 1], place[u + 1 : u + 2]),
            )
            for i in range(2):
                hot[i].append(jnp.where(target == spots[i], 1.0, 0.0).astype(BF16))
        for i in range(2):
            acc[i] = acc[i] + dot_nt(jnp.concatenate(lhs[i], axis=1), jnp.concatenate(hot[i], axis=1))
    placed[:, 0:per] = acc[0]
    placed[:, per:total] = acc[1]
    each = 2 * Q_DEV
    for z in range(owners):
        spots = (z * Q_DEV, per + z * Q_DEV)
        pieces = [placed[8 * g : 8 * g + 8, at : at + Q_DEV] for g in range(3) for at in spots]
        wide = jnp.concatenate(pieces + [jnp.zeros((8, LANES - 3 * each), F32)], axis=1)
        messages[ring.index(z)] = wide.astype(BF16)


def spread_body(ring, arrived, copies, joined):
    owners = arrived.shape[0]
    each = 2 * Q_DEV
    for z in range(owners):
        message = arrived[ring.index(z)].astype(F32)
        for g in range(3):
            joined[8 * g : 8 * g + 8, z * each : (z + 1) * each] = message[:, g * each : (g + 1) * each]
    whole = joined[...].astype(BF16)
    for c in range(copies.shape[0]):
        copies[c] = whole


def finish_body(around, pieces, feat, logit, box, rows):
    owners = pieces.shape[2] // (2 * Q_DEV)
    total = pieces.shape[2]
    chips = pieces.shape[0]
    parts = [
        jnp.concatenate(
            [pieces[around.index(c), 0:16, :] for c in range(h * chips // 2, (h + 1) * chips // 2)], axis=0
        )
        for h in range(2)
    ]
    parts.append(jnp.concatenate([pieces[around.index(c), 16:24, :] for c in range(chips)], axis=0))
    images = 2 * owners

    def reorder(h):
        turned = parts[h].astype(F32).T
        for z in range(owners):
            for i in range(2):
                done = 0
                while done < Q_DEV:
                    at = z * 2 * Q_DEV + i * Q_DEV + done
                    n = min(8 - at % 8, Q_DEV - done)
                    rows[h, pl.ds(done * images + 2 * z + i, n, stride=images), :] = turned[at : at + n]
                    done += n

    for h in range(3):
        reorder(h)
    for h in range(2):
        feat[:, h * LANES : (h + 1) * LANES] = rows[h].astype(BF16)
    rest = rows[2].astype(BF16)
    logit[...] = rest[:, 0:CLS]
    boxes = rows[2].T[CLS : CLS + KEYS].astype(BF16)
    for r in range(Q_DEV):
        box[r] = boxes[:, r * images : (r + 1) * images]


def token_body(cols_axis, map_w, map_h, steps, first, last, shard, after, memory, *refs):
    weights, (logit, box, logit_part, box_part, sems) = refs[:12], refs[-5:]
    per = TOK // BLOCK

    def sends(k):
        step = first[0] + k
        image = jnp.where(step >= per, 1, 0)
        at = pl.multiple_of((step - image * per) * BLOCK, BLOCK)
        return (
            pltpu.make_async_copy(logit_part.at[k], logit.at[image, :, pl.ds(at, BLOCK)], sems.at[0, k]),
            pltpu.make_async_copy(box_part.at[k], box.at[image, :, pl.ds(at, BLOCK)], sems.at[1, k]),
        )

    for k in range(steps):

        @pl.when((pl.program_id(0) == k) & (first[0] + k < last[0]))
        def _():
            step = first[0] + k
            local = jnp.where(step >= per, step - per, step)
            token = local * BLOCK + lax.broadcasted_iota(jnp.int32, (1, BLOCK), 1)
            prior = prior_logits(token, shard[0], map_w, map_h, cols_axis)
            _, logits, boxes = heads(memory[0], *weights, prior)
            logit_part[k] = logits
            box_part[k] = boxes
            for send in sends(k):
                send.start()

    @pl.when(pl.program_id(0) == steps - 1)
    def _():
        for k in range(steps):

            @pl.when(first[0] + k < last[0])
            def _():
                for send in sends(k):
                    send.wait()


def token_heads(geometry, first, last, steps, shard, after, memory, weights, *earlier):
    per = TOK // BLOCK

    def rows(j, first, last, shard):
        step = jnp.minimum(first[0] + j, jnp.maximum(last[0] - 1, 0))
        image = jnp.where(step >= per, 1, 0)
        return image, step - image * per, 0

    full = lambda a: pl.BlockSpec(a.shape, lambda j, first, last, shard: (0,) * a.ndim)
    return pl.pallas_call(
        lambda *refs: token_body(*geometry, steps, *refs),
        out_shape=(
            jax.ShapeDtypeStruct((2, CLS, TOK), BF16),
            jax.ShapeDtypeStruct((2, KEYS, TOK), F32),
        ),
        grid_spec=pltpu.PrefetchScalarGridSpec(
            num_scalar_prefetch=3,
            grid=(steps,),
            in_specs=[ANY, pl.BlockSpec((1, BLOCK, D), rows)]
            + [VMEM if k in BIG else full(w) for k, w in enumerate(weights[:-1])]
            + [SMEM]
            + [ANY] * len(earlier),
            out_specs=(ANY, ANY),
            scratch_shapes=[
                pltpu.VMEM((steps, CLS, BLOCK), BF16),
                pltpu.VMEM((steps, KEYS, BLOCK), F32),
                pltpu.SemaphoreType.DMA((2, steps)),
            ],
        ),
        input_output_aliases={17: 0, 18: 1} if earlier else {},
        cost_estimate=pl.CostEstimate(flops=1_300_000_000, transcendentals=30_000, bytes_accessed=1_200_000),
        name="token_heads",
    )(first, last, shard, after, memory, *weights, *earlier)


def shards(
    memory,
    enc_weight,
    enc_bias,
    norm_gain,
    norm_bias,
    class_weight,
    class_bias,
    box_w1,
    box_b1,
    box_w2,
    box_b2,
    box_w3,
    box_b3,
    picked,
    counts,
):
    owners = lax.axis_size("img")
    cols_axis = lax.axis_size("sx")
    cores = lax.axis_size("sy_1")
    chips = lax.axis_size("sy_0") * cols_axis
    map_w = float(TILE_W * cols_axis)
    map_h = float(TILE_H * lax.axis_size("sy_0") * cores)
    shard = lax.axis_index(PLANE).astype(jnp.int32).reshape(1)
    row = lambda v: v.reshape(1, -1)
    weights = (
        enc_weight,
        row(enc_bias),
        row(norm_gain),
        row(norm_bias),
        class_weight.T,
        row(class_bias),
        box_w1,
        row(box_b1),
        box_w2,
        row(box_b2),
        box_w3.T,
        box_b3,
    )
    geometry = (cols_axis, map_w, map_h)
    tiles = plane_order(chips, cores, cols_axis)
    around = plane_order(chips, 1, cols_axis)
    ring = rolled(owners, 5 * owners // 8)
    blocks = 2 * TOK // BLOCK
    quarter = lax.axis_index("img") * 4 // owners
    aside = lambda axis: jnp.abs(lax.axis_index(axis) - lax.axis_size(axis) // 2)
    far = aside("sy_0") + aside("sx") >= 3
    late = jnp.where(far, 1, 2)
    middle = jnp.where(quarter == 0, blocks, jnp.where(quarter == 1, blocks * 3 // 4, late))
    edges = [jnp.asarray(e, jnp.int32).reshape(1) for e in (0, middle, blocks)]
    close = tuple(near(w) if k in BIG else w for k, w in enumerate(weights))

    def heads_of(k, after, *earlier):
        steps = (blocks, blocks - 1)[k]
        return token_heads(geometry, edges[k], edges[k + 1], steps, shard, after, memory, close, *earlier)

    payload = pl.pallas_call(
        lambda *refs: select_body(*geometry, chips, cores, tiles, *refs),
        out_shape=jax.ShapeDtypeStruct((chips * cores, ROWS, LANES), BF16),
        in_specs=[SMEM, SMEM, SMEM, VMEM, ANY] + [ANY if w in BIG else VMEM for w in range(11)] + [SMEM],
        out_specs=ANY,
        scratch_shapes=[pltpu.VMEM((2 * MOST * 16, D), BF16)]
        + [pltpu.VMEM(weights[w].shape, BF16) for w in BIG]
        + [pltpu.VMEM((chips * cores, ROWS, LANES), BF16)]
        + [pltpu.SemaphoreType.DMA, pltpu.SemaphoreType.DMA((len(BIG),))],
        name="select_rows",
    )(picked, counts.T, shard, picked, memory, *weights)
    received = lax.all_to_all(payload, PLANE, 0, 0, axis_index_groups=[tiles], tiled=True)
    tokens = heads_of(0, payload)
    total = owners * 2 * Q_DEV
    messages = pl.pallas_call(
        lambda *refs: place_body(owners, tiles, ring, *refs),
        out_shape=pltpu.VMEM((owners, 8, LANES), BF16),
        in_specs=[VMEM, ANY],
        out_specs=VMEM,
        scratch_shapes=[pltpu.VMEM((ROWS, total), F32)],
        name="place_rows",
    )(near(received), tokens[1])
    arrived = lax.all_to_all(messages, "img", 0, 0, axis_index_groups=[ring], tiled=True)
    copies = pl.pallas_call(
        lambda *refs: spread_body(ring, *refs),
        out_shape=pltpu.VMEM((chips, ROWS, total), BF16),
        in_specs=[VMEM],
        out_specs=VMEM,
        scratch_shapes=[pltpu.VMEM((ROWS, total), F32)],
        name="spread_rows",
    )(near(arrived))
    pieces = lax.all_to_all(copies, CHIPS, 0, 0, axis_index_groups=[around], tiled=True)
    token_logits, token_boxes = heads_of(1, copies, *tokens)
    feat, logit, box = pl.pallas_call(
        lambda *refs: finish_body(around, *refs),
        out_shape=(
            jax.ShapeDtypeStruct((total, D), BF16),
            jax.ShapeDtypeStruct((total, CLS), BF16),
            jax.ShapeDtypeStruct((Q_DEV, KEYS, 2 * owners), BF16),
        ),
        in_specs=[VMEM],
        out_specs=(VMEM, VMEM, VMEM),
        scratch_shapes=[pltpu.VMEM((3, total, LANES), F32)],
        name="finish_rows",
    )(near(pieces))
    owned = lambda a: jnp.transpose(a.reshape(Q_DEV, 2 * owners, -1), (1, 0, 2))
    return (token_logits, token_boxes, owned(feat), owned(logit), jnp.transpose(box, (2, 0, 1)))


def solution(mesh):
    finer = Mesh(
        mesh.devices.reshape(mesh.shape["img"], 4, 2, mesh.shape["sx"]),
        ("img", "sy_0", "sy_1", "sx"),
    )
    in_specs = (
        (P("img", PLANE, None),) + (P(),) * 12 + (P("img", PLANE), P("img", PLANE))
    )
    out_specs = (
        P("img", None, PLANE),
        P("img", None, PLANE),
        P(None, "img", None),
        P(None, "img", None),
        P(None, "img", None),
    )
    return jax.shard_map(
        shards, mesh=finer, in_specs=in_specs, out_specs=out_specs, check_vma=False
    )
```

```python
import jax
import jax.numpy as jnp
from jax import lax
from jax.experimental import pallas as pl
from jax.experimental.pallas import tpu as pltpu
from jax.sharding import Mesh
from jax.sharding import PartitionSpec as P

TILE_H = 40
TILE_W = 64
D = 256
CLS = 91
KEYS = 4
MOST = 40
TOK = 2560
Q_DEV = 20
LANES = 128
HALF = 64
MARK = 120
ROWS = 24
BLOCK = 1280
PLANE = ("sy_0", "sy_1", "sx")
CHIPS = ("sy_0", "sx")
F32 = jnp.float32
BF16 = jnp.bfloat16
VMEM = pl.BlockSpec(memory_space=pltpu.VMEM)
SMEM = pl.BlockSpec(memory_space=pltpu.SMEM)
ANY = pl.BlockSpec(memory_space=pl.ANY)
BIG = (0, 4, 6, 8, 10)
NT = (((1,), (1,)), ((), ()))


def rolled(n, first):
    return [(first + k) % n for k in range(n)]


def plane_order(chips, cores, cols_axis):
    rows_axis = chips // cols_axis
    order = []
    for hi in rolled(rows_axis, rows_axis // 2):
        for core in rolled(cores, cores // 2):
            for lo in rolled(cols_axis, cols_axis // 2):
                order.append((hi * cores + core) * cols_axis + lo)
    return order


def near(x):
    return pltpu.with_memory_space_constraint(x, pltpu.VMEM)


def dot(a, b):
    return jnp.dot(a, b, preferred_element_type=F32)


def dot_nt(a, b):
    return lax.dot_general(a, b, NT, preferred_element_type=F32)


def column(v):
    n = v.shape[1]
    if n < LANES:
        v = jnp.concatenate([v, jnp.zeros((1, LANES - n), F32)], axis=1)
    return jnp.broadcast_to(v, (LANES, LANES)).T


def heads_split(x, enc_w, enc_b, gain, bias, cls_t, cls_b, w1, b1, w2, b2, w3_t, b3, prior_logit):
    pre = dot(x, enc_w[...]) + enc_b[...]
    mean = jnp.mean(pre, axis=-1, keepdims=True)
    centered = pre - mean
    var = jnp.mean(centered * centered, axis=-1, keepdims=True)
    out = (centered * lax.rsqrt(var + 1e-05) * gain[...] + bias[...]).astype(BF16)
    yield out
    n = x.shape[0]
    cls_col = column(cls_b[...])[:CLS]
    if n > LANES:
        cls_col = jnp.concatenate([cls_col] * (n // LANES), axis=1)
    logits = (dot_nt(cls_t[...], out) + cls_col).astype(BF16)
    hidden = jnp.maximum(dot(out, w1[...]) + b1[...], 0.0).astype(BF16)
    hidden = jnp.maximum(dot(hidden, w2[...]) + b2[...], 0.0).astype(BF16)
    which = lax.broadcasted_iota(jnp.int32, (KEYS, n), 0)
    b3_col = jnp.where(which == 0, b3[0], jnp.where(which == 1, b3[1], jnp.where(which == 2, b3[2], b3[3])))
    delta = dot_nt(w3_t[...], hidden) + b3_col
    boxes = jax.nn.sigmoid(delta + prior_logit)
    yield logits, boxes


def heads(*args):
    out, (logits, boxes) = heads_split(*args)
    return out, logits, boxes


def prior_logits(token, shard, map_w, map_h, cols_axis):
    row = shard // cols_axis * TILE_H + (token >> 6)
    col = shard % cols_axis * TILE_W + (token & 63)
    center_x = (col.astype(F32) + 0.5) / map_w
    center_y = (row.astype(F32) + 0.5) / map_h
    n = token.shape[1]
    which = lax.broadcasted_iota(jnp.int32, (4, n), 0)
    prior = jnp.where(which == 0, center_x, jnp.where(which == 1, center_y, 0.05))
    return jnp.log(prior / (1.0 - prior))


def select_body(cols_axis, map_w, map_h, chips, cores, order, picked, counts, shard, pick_vec, memory, *refs):
    weights, payload, tiles = list(refs[:12]), refs[12], refs[13]
    near_weights, staged, sem, sems = refs[14:-3], refs[-3], refs[-2], refs[-1]
    for i in range(2):
        for k in range(MOST):
            base = pl.multiple_of((picked[i, k] >> 4) << 4, 16)
            j = i * MOST + k
            pltpu.make_async_copy(memory.at[i, pl.ds(base, 16), :], tiles.at[pl.ds(16 * j, 16), :], sem).start()
    loads = [pltpu.make_async_copy(weights[w], near_weights[k], sems.at[k]) for k, w in enumerate(BIG)]
    for load in loads:
        load.start()
    for k, w in enumerate(BIG):
        weights[w] = near_weights[k]
    n = 2 * MOST * 16
    row = lax.broadcasted_iota(jnp.int32, (LANES, n), 0)
    col = lax.broadcasted_iota(jnp.int32, (LANES, n), 1)
    pick = pick_vec[...]
    gap = jnp.zeros((1, HALF - MOST), jnp.int32)
    pick = jnp.concatenate([pick[0:1], gap, pick[1:2], gap], axis=1)
    pick_col = column((pick & 15).astype(F32)).astype(jnp.int32)
    pick_col = jnp.concatenate([pick_col] * (n // LANES), axis=1)
    used = (row & (HALF - 1)) < MOST
    source = jnp.where(row < HALF, row, row - (HALF - MOST)) * 16
    chosen = used & (col == source + pick_col)
    chosen = jnp.where(chosen, 1.0, 0.0).astype(BF16)
    prior = prior_logits(pick, shard[0], map_w, map_h, cols_axis)
    pltpu.make_async_copy(memory.at[0, pl.ds(0, n), :], tiles, sem).wait()
    for load in loads:
        load.wait()
    x = dot(chosen, tiles[...]).astype(BF16)
    c0 = counts[0, 0].astype(F32)
    c1 = counts[0, 1].astype(F32)

    def marked(v):
        lane = lax.broadcasted_iota(jnp.int32, v.shape, 1)
        return jnp.where(lane == MARK, c0, jnp.where(lane == MARK + 1, c1, v)).astype(BF16)

    def stage(rows, at, each):
        for hi in range(chips // cols_axis):
            for lo in range(cols_axis):
                c = hi * cols_axis + lo
                for core in range(cores):
                    k = order.index((hi * cores + core) * cols_axis + lo)
                    staged[k, at : at + each, :] = rows[each * c : each * c + each, :]

    parts = heads_split(x, *weights, prior)
    stage(marked(next(parts).astype(F32).T), 0, 16)
    feats = pltpu.make_async_copy(staged.at[:, 0:16, :], payload.at[:, 0:16, :], sems.at[0])
    feats.start()
    logits, boxes = next(parts)
    rest = [logits.astype(F32), boxes.astype(F32), jnp.zeros((LANES - CLS - KEYS, LANES), F32)]
    stage(marked(jnp.concatenate(rest, axis=0)), 16, 8)
    others = pltpu.make_async_copy(staged.at[:, 16:24, :], payload.at[:, 16:24, :], sems.at[1])
    others.start()
    feats.wait()
    others.wait()


def place_body(owners, tiles, ring, received, after, messages, placed):
    shards = received.shape[0]
    at = [tiles.index(t) for t in range(shards)]
    flat = jnp.concatenate([received[k] for k in at], axis=0)
    r = lax.broadcasted_iota(jnp.int32, (2 * shards, shards * ROWS), 0)
    m = lax.broadcasted_iota(jnp.int32, (2 * shards, shards * ROWS), 1)
    tile = (m * 2731) >> 16
    wanted = ((r < shards) & (tile == r)) | (tile < r - shards)
    take = jnp.where(wanted & (m == tile * ROWS), 1.0, 0.0)
    res = dot(take.astype(BF16), flat)
    count, start = res[:shards], res[shards:]
    lane = lax.broadcasted_iota(jnp.int32, (shards, LANES), 1)
    image = jnp.where(lane < HALF, 0, 1)
    step = lane - image * HALF
    pick = lambda a: jnp.where(lane < HALF, a[:, MARK : MARK + 1], a[:, MARK + 1 : MARK + 2]).astype(jnp.int32)
    slot = pick(start) + step
    valid = (step < pick(count)) & (step < MOST)
    place = jnp.where(valid, slot, -1)
    swapped = pltpu.roll(place, HALF, 1)
    per = owners * Q_DEV
    total = 2 * per
    target = lax.broadcasted_iota(jnp.int32, (per, LANES), 0)
    low = lax.broadcasted_iota(jnp.int32, (1, LANES), 1) < HALF
    low_rows = lax.broadcasted_iota(jnp.int32, (ROWS, LANES), 1) < HALF
    acc = [jnp.zeros((ROWS, per), F32) for _ in range(2)]
    for t in range(0, shards, 4):
        lhs, hot = [[], []], [[], []]
        for u in (t, t + 2):
            a, b = (received[at[v]].astype(F32) for v in (u, u + 1))
            a_swapped, b_swapped = pltpu.roll(a, HALF, 1), pltpu.roll(b, HALF, 1)
            lhs[0].append(jnp.where(low_rows, a, b_swapped).astype(BF16))
            lhs[1].append(jnp.where(low_rows, a_swapped, b).astype(BF16))
            spots = (
                jnp.where(low, place[u : u + 1], swapped[u + 1 : u + 2]),
                jnp.where(low, swapped[u : u + 1], place[u + 1 : u + 2]),
            )
            for i in range(2):
                hot[i].append(jnp.where(target == spots[i], 1.0, 0.0).astype(BF16))
        for i in range(2):
            acc[i] = acc[i] + dot_nt(jnp.concatenate(lhs[i], axis=1), jnp.concatenate(hot[i], axis=1))
    placed[:, 0:per] = acc[0]
    placed[:, per:total] = acc[1]
    each = 2 * Q_DEV
    for z in range(owners):
        spots = (z * Q_DEV, per + z * Q_DEV)
        pieces = [placed[8 * g : 8 * g + 8, at : at + Q_DEV] for g in range(3) for at in spots]
        wide = jnp.concatenate(pieces + [jnp.zeros((8, LANES - 3 * each), F32)], axis=1)
        messages[ring.index(z)] = wide.astype(BF16)


def spread_body(ring, arrived, copies, joined):
    owners = arrived.shape[0]
    each = 2 * Q_DEV
    for z in range(owners):
        message = arrived[ring.index(z)].astype(F32)
        for g in range(3):
            joined[8 * g : 8 * g + 8, z * each : (z + 1) * each] = message[:, g * each : (g + 1) * each]
    whole = joined[...].astype(BF16)
    for c in range(copies.shape[0]):
        copies[c] = whole


def finish_body(around, pieces, feat, logit, box, rows):
    owners = pieces.shape[2] // (2 * Q_DEV)
    total = pieces.shape[2]
    chips = pieces.shape[0]
    parts = [
        jnp.concatenate(
            [pieces[around.index(c), 0:16, :] for c in range(h * chips // 2, (h + 1) * chips // 2)], axis=0
        )
        for h in range(2)
    ]
    parts.append(jnp.concatenate([pieces[around.index(c), 16:24, :] for c in range(chips)], axis=0))
    images = 2 * owners

    def reorder(h):
        turned = parts[h].astype(F32).T
        for z in range(owners):
            for i in range(2):
                done = 0
                while done < Q_DEV:
                    at = z * 2 * Q_DEV + i * Q_DEV + done
                    n = min(8 - at % 8, Q_DEV - done)
                    rows[h, pl.ds(done * images + 2 * z + i, n, stride=images), :] = turned[at : at + n]
                    done += n

    for h in range(3):
        reorder(h)
    for h in range(2):
        feat[:, h * LANES : (h + 1) * LANES] = rows[h].astype(BF16)
    rest = rows[2].astype(BF16)
    logit[...] = rest[:, 0:CLS]
    boxes = rows[2].T[CLS : CLS + KEYS].astype(BF16)
    for r in range(Q_DEV):
        box[r] = boxes[:, r * images : (r + 1) * images]


def token_body(cols_axis, map_w, map_h, steps, first, last, shard, after, memory, *refs):
    weights, (logit, box, logit_part, box_part, sems) = refs[:12], refs[-5:]
    per = TOK // BLOCK

    def sends(k):
        step = first[0] + k
        image = jnp.where(step >= per, 1, 0)
        at = pl.multiple_of((step - image * per) * BLOCK, BLOCK)
        return (
            pltpu.make_async_copy(logit_part.at[k], logit.at[image, :, pl.ds(at, BLOCK)], sems.at[0, k]),
            pltpu.make_async_copy(box_part.at[k], box.at[image, :, pl.ds(at, BLOCK)], sems.at[1, k]),
        )

    for k in range(steps):

        @pl.when((pl.program_id(0) == k) & (first[0] + k < last[0]))
        def _():
            step = first[0] + k
            local = jnp.where(step >= per, step - per, step)
            token = local * BLOCK + lax.broadcasted_iota(jnp.int32, (1, BLOCK), 1)
            prior = prior_logits(token, shard[0], map_w, map_h, cols_axis)
            _, logits, boxes = heads(memory[0], *weights, prior)
            logit_part[k] = logits
            box_part[k] = boxes
            for send in sends(k):
                send.start()

    @pl.when(pl.program_id(0) == steps - 1)
    def _():
        for k in range(steps):

            @pl.when(first[0] + k < last[0])
            def _():
                for send in sends(k):
                    send.wait()


def token_heads(geometry, first, last, steps, shard, after, memory, weights, *earlier):
    per = TOK // BLOCK

    def rows(j, first, last, shard):
        step = jnp.minimum(first[0] + j, jnp.maximum(last[0] - 1, 0))
        image = jnp.where(step >= per, 1, 0)
        return image, step - image * per, 0

    full = lambda a: pl.BlockSpec(a.shape, lambda j, first, last, shard: (0,) * a.ndim)
    return pl.pallas_call(
        lambda *refs: token_body(*geometry, steps, *refs),
        out_shape=(
            jax.ShapeDtypeStruct((2, CLS, TOK), BF16),
            jax.ShapeDtypeStruct((2, KEYS, TOK), F32),
        ),
        grid_spec=pltpu.PrefetchScalarGridSpec(
            num_scalar_prefetch=3,
            grid=(steps,),
            in_specs=[ANY, pl.BlockSpec((1, BLOCK, D), rows)]
            + [VMEM if k in BIG else full(w) for k, w in enumerate(weights[:-1])]
            + [SMEM]
            + [ANY] * len(earlier),
            out_specs=(ANY, ANY),
            scratch_shapes=[
                pltpu.VMEM((steps, CLS, BLOCK), BF16),
                pltpu.VMEM((steps, KEYS, BLOCK), F32),
                pltpu.SemaphoreType.DMA((2, steps)),
            ],
        ),
        input_output_aliases={17: 0, 18: 1} if earlier else {},
        cost_estimate=pl.CostEstimate(flops=1_300_000_000, transcendentals=30_000, bytes_accessed=1_200_000),
        name="token_heads",
    )(first, last, shard, after, memory, *weights, *earlier)


def shards(
    memory,
    enc_weight,
    enc_bias,
    norm_gain,
    norm_bias,
    class_weight,
    class_bias,
    box_w1,
    box_b1,
    box_w2,
    box_b2,
    box_w3,
    box_b3,
    picked,
    counts,
):
    owners = lax.axis_size("img")
    cols_axis = lax.axis_size("sx")
    cores = lax.axis_size("sy_1")
    chips = lax.axis_size("sy_0") * cols_axis
    map_w = float(TILE_W * cols_axis)
    map_h = float(TILE_H * lax.axis_size("sy_0") * cores)
    shard = lax.axis_index(PLANE).astype(jnp.int32).reshape(1)
    row = lambda v: v.reshape(1, -1)
    weights = (
        enc_weight,
        row(enc_bias),
        row(norm_gain),
        row(norm_bias),
        class_weight.T,
        row(class_bias),
        box_w1,
        row(box_b1),
        box_w2,
        row(box_b2),
        box_w3.T,
        box_b3,
    )
    geometry = (cols_axis, map_w, map_h)
    tiles = plane_order(chips, cores, cols_axis)
    around = plane_order(chips, 1, cols_axis)
    ring = rolled(owners, 5 * owners // 8)
    blocks = 2 * TOK // BLOCK
    quarter = lax.axis_index("img") * 4 // owners
    aside = lambda axis: jnp.abs(lax.axis_index(axis) - lax.axis_size(axis) // 2)
    far = aside("sy_0") + aside("sx") >= 3
    late = jnp.where(far, 1, 2)
    middle = jnp.where(quarter == 0, blocks, jnp.where(quarter == 1, blocks * 3 // 4, late))
    edges = [jnp.asarray(e, jnp.int32).reshape(1) for e in (0, middle, blocks)]
    close = tuple(near(w) if k in BIG else w for k, w in enumerate(weights))

    def heads_of(k, after, *earlier):
        steps = (blocks, blocks - 1)[k]
        return token_heads(geometry, edges[k], edges[k + 1], steps, shard, after, memory, close, *earlier)

    payload = pl.pallas_call(
        lambda *refs: select_body(*geometry, chips, cores, tiles, *refs),
        out_shape=jax.ShapeDtypeStruct((chips * cores, ROWS, LANES), BF16),
        in_specs=[SMEM, SMEM, SMEM, VMEM, ANY] + [ANY if w in BIG else VMEM for w in range(11)] + [SMEM],
        out_specs=ANY,
        scratch_shapes=[pltpu.VMEM((2 * MOST * 16, D), BF16)]
        + [pltpu.VMEM(weights[w].shape, BF16) for w in BIG]
        + [pltpu.VMEM((chips * cores, ROWS, LANES), BF16)]
        + [pltpu.SemaphoreType.DMA, pltpu.SemaphoreType.DMA((len(BIG),))],
        name="select_rows",
    )(picked, counts.T, shard, picked, memory, *weights)
    received = lax.all_to_all(payload, PLANE, 0, 0, axis_index_groups=[tiles], tiled=True)
    tokens = heads_of(0, payload)
    total = owners * 2 * Q_DEV
    messages = pl.pallas_call(
        lambda *refs: place_body(owners, tiles, ring, *refs),
        out_shape=pltpu.VMEM((owners, 8, LANES), BF16),
        in_specs=[VMEM, ANY],
        out_specs=VMEM,
        scratch_shapes=[pltpu.VMEM((ROWS, total), F32)],
        name="place_rows",
    )(near(received), tokens[1])
    arrived = lax.all_to_all(messages, "img", 0, 0, axis_index_groups=[ring], tiled=True)
    copies = pl.pallas_call(
        lambda *refs: spread_body(ring, *refs),
        out_shape=pltpu.VMEM((chips, ROWS, total), BF16),
        in_specs=[VMEM],
        out_specs=VMEM,
        scratch_shapes=[pltpu.VMEM((ROWS, total), F32)],
        name="spread_rows",
    )(near(arrived))
    pieces = lax.all_to_all(copies, CHIPS, 0, 0, axis_index_groups=[around], tiled=True)
    token_logits, token_boxes = heads_of(1, copies, *tokens)
    feat, logit, box = pl.pallas_call(
        lambda *refs: finish_body(around, *refs),
        out_shape=(
            jax.ShapeDtypeStruct((total, D), BF16),
            jax.ShapeDtypeStruct((total, CLS), BF16),
            jax.ShapeDtypeStruct((Q_DEV, KEYS, 2 * owners), BF16),
        ),
        in_specs=[VMEM],
        out_specs=(VMEM, VMEM, VMEM),
        scratch_shapes=[pltpu.VMEM((3, total, LANES), F32)],
        name="finish_rows",
    )(near(pieces))
    owned = lambda a: jnp.transpose(a.reshape(Q_DEV, 2 * owners, -1), (1, 0, 2))
    return (token_logits, token_boxes, owned(feat), owned(logit), jnp.transpose(box, (2, 0, 1)))


def solution(mesh):
    finer = Mesh(
        mesh.devices.reshape(mesh.shape["img"], 4, 2, mesh.shape["sx"]),
        ("img", "sy_0", "sy_1", "sx"),
    )
    in_specs = (
        (P("img", PLANE, None),) + (P(),) * 12 + (P("img", PLANE), P("img", PLANE))
    )
    out_specs = (
        P("img", None, PLANE),
        P("img", None, PLANE),
        P(None, "img", None),
        P(None, "img", None),
        P(None, "img", None),
    )
    return jax.shard_map(
        shards, mesh=finer, in_specs=in_specs, out_specs=out_specs, check_vma=False
    )
```
